8 devices in a mesh: etp: 2 (over z, y), ep: 4 (over x, core).
Axes of the slice: x: 2, y: 2, z: 1, core: 2. Of those that a mesh axis runs over, the one named last changes fastest.
Arguments:
- hidden: bfloat16 [16384, 512], P(('ep', 'etp'))
- w_router: float32 [512, 32], replicated
- expert_ids: int32 [16384, 2], P(('ep', 'etp'))
- d_out: bfloat16 [16384, 512], P(('ep', 'etp'))
- w_gate: bfloat16 [32, 512, 768], P('ep', None, 'etp')
- w_up: bfloat16 [32, 512, 768], P('ep', None, 'etp')
- w_down: bfloat16 [32, 768, 512], P('ep', 'etp')
Outputs:
- output 1: bfloat16 [16384, 512], P(('ep', 'etp'))
- output 2: bfloat16 [16384, 512], P(('ep', 'etp'))
- output 3: float32 [512, 32], replicated
- output 4: float32 [], replicated
- output 5: float32 [32, 512, 768], P('ep', None, 'etp')
- output 6: float32 [32, 512, 768], P('ep', None, 'etp')
- output 7: float32 [32, 768, 512], P('ep', 'etp')
All inputs are finite; a program needn't handle non-finite values.
Results may differ from the reference program's by a relative error of at most 0.00900198.
Values are sent between devices in bfloat16 or wider.
A program may use at most 1 GiB of HBM per device.

```python
import jax
import jax.numpy as jnp
from jax import lax

EXPERTS = 32
D_MODEL = 512
D_FF = 768
TOKENS = 16384
N_DEVICES = 8

CAPACITY = (5 * TOKENS + 2 * EXPERTS - 1) // (2 * EXPERTS)
BLOCK_TOKENS = TOKENS // N_DEVICES


def draw_choices(draw_key):
    quarter = BLOCK_TOKENS // (2 * EXPERTS)
    perm_key, block_key = jax.random.split(draw_key)
    expert_order = jax.random.permutation(perm_key, EXPERTS)
    hot_shift = jnp.zeros((EXPERTS,), jnp.int32).at[:4].set(jnp.array([2, 2, -2, -2], jnp.int32) * quarter)

    def one_block(one_key):
        k_noise, k_rows, k_flip = jax.random.split(one_key, 3)
        count_noise = jax.random.randint(k_noise, (EXPERTS,), 0, quarter + 1)
        count_noise = count_noise.at[0].set(quarter).at[1].set(0)
        count_perm = 4 * quarter + count_noise - jnp.roll(count_noise, -1) + hot_shift
        counts = jnp.zeros((EXPERTS,), jnp.int32).at[expert_order].set(count_perm)
        ends = jnp.cumsum(counts)
        id_seq = jnp.sum(jnp.arange(2 * BLOCK_TOKENS)[:, None] >= ends[None, :], axis=1).astype(jnp.int32)
        id_pairs = jnp.stack([id_seq[:BLOCK_TOKENS], id_seq[BLOCK_TOKENS:]], axis=1)
        id_pairs = id_pairs[jax.random.permutation(k_rows, BLOCK_TOKENS)]
        flip_mask = jax.random.randint(k_flip, (BLOCK_TOKENS, 1), 0, 2) == 1
        return jnp.where(flip_mask, id_pairs[:, ::-1], id_pairs)

    blocks = jax.vmap(one_block)(jax.random.split(block_key, N_DEVICES))
    return blocks.reshape(TOKENS, 2)


def setup_inputs(seed: int = 0) -> dict:
    root_key = jax.random.key(seed)
    k_hid, k_route, k_ids, k_dout, k_gate, k_up, k_down = jax.random.split(root_key, 7)
    hidden = jax.random.normal(k_hid, (TOKENS, D_MODEL), jnp.float32).astype(jnp.bfloat16)
    w_router = jax.random.normal(k_route, (D_MODEL, EXPERTS), jnp.float32) * (0.5 * D_MODEL ** -0.5)
    expert_ids = draw_choices(k_ids)
    d_out = jax.random.normal(k_dout, (TOKENS, D_MODEL), jnp.float32).astype(jnp.bfloat16)
    w_gate = (jax.random.normal(k_gate, (EXPERTS, D_MODEL, D_FF), jnp.float32) * D_MODEL ** -0.5).astype(jnp.bfloat16)
    w_up = (jax.random.normal(k_up, (EXPERTS, D_MODEL, D_FF), jnp.float32) * D_MODEL ** -0.5).astype(jnp.bfloat16)
    w_down = (jax.random.normal(k_down, (EXPERTS, D_FF, D_MODEL), jnp.float32) * D_FF ** -0.5).astype(jnp.bfloat16)
    return {"hidden": hidden, "w_router": w_router, "expert_ids": expert_ids, "d_out": d_out, "w_gate": w_gate, "w_up": w_up, "w_down": w_down}


def route_terms(logits, expert_ids):
    prob_vals = jax.nn.softmax(logits, axis=-1)
    picked = jnp.take_along_axis(prob_vals, expert_ids, axis=1)
    return picked / jnp.sum(picked, axis=1, keepdims=True), jnp.sum(prob_vals, axis=0)


def expert_pass(operands):
    x_buf, dy_buf, gate_w, up_w, down_w = operands
    act_a = jnp.dot(x_buf, gate_w, preferred_element_type=jnp.float32)
    act_b = jnp.dot(x_buf, up_w, preferred_element_type=jnp.float32)
    sig_a = jax.nn.sigmoid(act_a)
    silu_a = act_a * sig_a
    inner_act = (silu_a * act_b).astype(jnp.bfloat16)
    y_buf = jnp.dot(inner_act, down_w, preferred_element_type=jnp.float32).astype(jnp.bfloat16)
    d_inner = jnp.dot(dy_buf, down_w.T, preferred_element_type=jnp.float32)
    d_act_a = (d_inner * act_b * sig_a * (1.0 + act_a * (1.0 - sig_a))).astype(jnp.bfloat16)
    d_act_b = (d_inner * silu_a).astype(jnp.bfloat16)
    dx_buf = (jnp.dot(d_act_a, gate_w.T, preferred_element_type=jnp.float32) + jnp.dot(d_act_b, up_w.T, preferred_element_type=jnp.float32)).astype(jnp.bfloat16)
    g_gate = jnp.dot(x_buf.T, d_act_a, preferred_element_type=jnp.float32)
    g_up = jnp.dot(x_buf.T, d_act_b, preferred_element_type=jnp.float32)
    g_down = jnp.dot(inner_act.T, dy_buf, preferred_element_type=jnp.float32)
    return y_buf, dx_buf, g_gate, g_up, g_down


def reference(hidden, w_router, expert_ids, d_out, w_gate, w_up, w_down):
    hidden_f = hidden.astype(jnp.float32)
    logits = jnp.dot(hidden_f, w_router, preferred_element_type=jnp.float32)
    (gate_vals, prob_sum), route_vjp = jax.vjp(lambda logit_in: route_terms(logit_in, expert_ids), logits)
    n_assign = 2 * TOKENS
    flat_ids = expert_ids.reshape(-1)
    assign = jnp.arange(n_assign, dtype=jnp.int32)
    counts = jnp.bincount(flat_ids, length=EXPERTS)
    sort_order = jnp.argsort(flat_ids * n_assign + assign)
    sort_rank = jnp.zeros((n_assign,), jnp.int32).at[sort_order].set(assign)
    starts = jnp.cumsum(counts) - counts
    slot_pos = sort_rank - starts[flat_ids]
    dest_rows = jnp.where(slot_pos < CAPACITY, flat_ids * CAPACITY + slot_pos, EXPERTS * CAPACITY)
    source = jnp.full((EXPERTS * CAPACITY,), n_assign, jnp.int32).at[dest_rows].set(assign, mode="drop")
    x_buf = jnp.take(hidden, source // 2, axis=0, mode="fill", fill_value=0).reshape(EXPERTS, CAPACITY, D_MODEL)
    d_mix = 2.0 * d_out.astype(jnp.float32)
    dy_assign = (gate_vals[:, :, None] * d_mix[:, None, :]).astype(jnp.bfloat16).reshape(n_assign, D_MODEL)
    dy_buf = jnp.take(dy_assign, source, axis=0, mode="fill", fill_value=0).reshape(EXPERTS, CAPACITY, D_MODEL)
    y_buf, dx_buf, g_gate, g_up, g_down = lax.map(expert_pass, (x_buf, dy_buf, w_gate, w_up, w_down))
    y_pair = jnp.take(y_buf.reshape(EXPERTS * CAPACITY, D_MODEL), dest_rows, axis=0, mode="fill", fill_value=0).reshape(TOKENS, 2, D_MODEL).astype(jnp.float32)
    dx_pair = jnp.take(dx_buf.reshape(EXPERTS * CAPACITY, D_MODEL), dest_rows, axis=0, mode="fill", fill_value=0).reshape(TOKENS, 2, D_MODEL).astype(jnp.float32)
    output = (hidden_f + 2.0 * jnp.sum(gate_vals[:, :, None] * y_pair, axis=1)).astype(jnp.bfloat16)
    d_gates = jnp.sum(d_mix[:, None, :] * y_pair, axis=2)
    route_frac = counts.astype(jnp.float32) / n_assign
    aux_loss = 0.01 * EXPERTS * jnp.sum(route_frac * prob_sum) / TOKENS
    (d_logits,) = route_vjp((d_gates, (0.01 * EXPERTS / TOKENS) * route_frac))
    d_router = jnp.dot(hidden_f.T, d_logits, preferred_element_type=jnp.float32)
    d_hidden = (d_out.astype(jnp.float32) + jnp.sum(dx_pair, axis=1) + jnp.dot(d_logits, w_router.T, preferred_element_type=jnp.float32)).astype(jnp.bfloat16)
    return output, d_hidden, d_router, aux_loss, g_gate, g_up, g_down
```

```python
import functools
import jax
import jax.numpy as jnp
from jax import lax
from jax.experimental import pallas as pl
from jax.experimental.pallas import tpu as pltpu
from jax.sharding import PartitionSpec as P

AUX_COEF = 0.01
OUT_SCALE = 2.0
CHUNKS = ((0, 2), (2, 4), (4, 6), (6, 8))

f32, bf16 = jnp.float32, jnp.bfloat16
TILE = 256
PAY_T = 40


def nn(a, b):
    return jnp.dot(a, b, preferred_element_type=f32)


def nt(a, b):
    return lax.dot_general(a, b, (((1,), (1,)), ((), ())), preferred_element_type=f32)


def tn(a, b):
    return lax.dot_general(a, b, (((0,), (0,)), ((), ())), preferred_element_type=f32)


def split3(v):
    hi = v.astype(bf16)
    rest = v - hi.astype(f32)
    mid = rest.astype(bf16)
    return hi, mid, (rest - mid.astype(f32)).astype(bf16)


def iota(shape, dim):
    return lax.broadcasted_iota(jnp.int32, shape, dim)


def params(**kw):
    return pltpu.CompilerParams(vmem_limit_bytes=60 * 2**20, **kw)


def cost(flops):
    return pl.CostEstimate(flops=int(flops), bytes_accessed=1 << 20, transcendentals=0)


def route_kernel(n_experts, h_ref, wr_ref, ids_ref, p_ref, code_ref, pay_ref):
    step = pl.program_id(0)

    @pl.when(step == 0)
    def _():
        pay_ref[...] = jnp.zeros_like(pay_ref)

    w_hi, w_mid, w_lo = split3(wr_ref[...])
    h = h_ref[...]
    z = (nn(h, w_lo) + nn(h, w_mid)) + nn(h, w_hi)
    z = jnp.exp(z - jnp.max(z, axis=1, keepdims=True))
    p = z / jnp.sum(z, axis=1, keepdims=True)
    p_ref[...] = p
    ids = ids_ref[...]
    lane = iota((TILE, n_experts), 1)
    e0, e1 = ids[:, 0:1], ids[:, 1:2]
    m0, m1 = lane == e0, lane == e1
    hist = jnp.where(m0 | m1, 1.0, 0.0).astype(f32)
    before = (iota((TILE, TILE), 1) < iota((TILE, TILE), 0)).astype(f32).astype(bf16)
    seen = pay_ref[n_experts:n_experts + 1, 0:n_experts]
    rank = nn(before, hist.astype(bf16)) + seen
    pick = lambda m, v: jnp.sum(jnp.where(m, v, 0.0), axis=1, keepdims=True)
    pos0, pos1 = pick(m0, rank), pick(m1, rank)
    p0, p1 = pick(m0, p), pick(m1, p)
    s = p0 + p1
    g0, g1 = p0 / s, p1 / s
    wide = iota((TILE, 128), 1)
    code = jnp.zeros((TILE, 128), f32)
    for k, v in enumerate((e0.astype(f32), e1.astype(f32), pos0, pos1, g0, g1, s)):
        code = jnp.where(wide == k, v, code)
    code_ref[...] = code
    pay_ref[pl.ds(pl.multiple_of(PAY_T + 8 * step, 8), 8), :] = code.T[0:8, :]
    slot = iota((TILE, 256), 1)
    gates = jnp.zeros((n_experts, 256), f32)
    for m, g, pos in ((m0, g0, pos0), (m1, g1, pos1)):
        one = (slot == pos.astype(jnp.int32)).astype(f32).astype(bf16)
        for piece in split3(jnp.where(m, g, 0.0)):
            gates = gates + tn(piece, one)
    pay_ref[0:n_experts, :] = pay_ref[0:n_experts, :] + gates
    pay_ref[n_experts:n_experts + 1, 0:n_experts] = seen + jnp.sum(hist, axis=0, keepdims=True)
    pay_ref[n_experts + 1:n_experts + 2, 0:n_experts] = (
        pay_ref[n_experts + 1:n_experts + 2, 0:n_experts] + jnp.sum(p, axis=0, keepdims=True))


def gather_kernel(capacity, slots, info_ref, cnt_ref, pay_ref, ha_ref, hb_ref, da_ref, db_ref,
                  x_ref, c_ref, m_ref):
    n_dev, n_experts = cnt_ref.shape
    local = pl.program_id(0)
    base = info_ref[2]
    expert = base + local
    expert_f = expert.astype(f32)
    tokens = ha_ref.shape[0]
    row = iota((slots, TILE), 0).astype(f32)
    for b, (h_ref, d_ref) in enumerate(((ha_ref, da_ref), (hb_ref, db_ref))):
        j = info_ref[b]
        prefix = jnp.sum(jnp.where(iota((n_dev, n_experts), 0) < j, cnt_ref[...], 0.0), axis=0, keepdims=True)
        room = jnp.sum(jnp.where(iota((1, n_experts), 1) == expert, capacity - prefix, 0.0), axis=1, keepdims=True)
        for i in range(tokens // TILE):
            t = pay_ref[j, PAY_T + 8 * i:PAY_T + 8 * i + 8, :]
            slot = jnp.where(t[0:1] == expert_f, t[2:3], jnp.where(t[1:2] == expert_f, t[3:4], -1.0))
            slot = jnp.where(slot < room, slot, -1.0)
            m_ref[:, i * TILE:(i + 1) * TILE] = jnp.where(row == slot, 1.0, 0.0).astype(bf16)
        m = m_ref[...]
        x_ref[0, b * slots:(b + 1) * slots, :] = nn(m, h_ref[...]).astype(bf16)
        d_rows = nn(m, d_ref[...])
        g = pay_ref[j, pl.ds(pl.multiple_of(base, 8), 8), :].T[0:slots, :]
        g = jnp.sum(jnp.where(iota((slots, 8), 1) == local, g, 0.0), axis=1, keepdims=True)
        c_ref[0, b * slots:(b + 1) * slots, :] = (g * (OUT_SCALE * d_rows)).astype(bf16)


def act(ab, du):
    ff = du.shape[1]
    a, b = ab[:, :ff], ab[:, ff:]
    sig = jax.nn.sigmoid(a)
    silu = a * sig
    u = (silu * b).astype(bf16)
    da = (du * b * sig * (1.0 + a * (1.0 - sig))).astype(bf16)
    db = (du * silu).astype(bf16)
    return u, jnp.concatenate([da, db], axis=1)


def grad_kernel(accumulate, xa_ref, xb_ref, ca_ref, cb_ref, w13_ref, w2_ref, *refs):
    g1_ref, g3_ref, g2_ref = refs[-3:]
    ff = w2_ref.shape[1]
    d13, d2 = None, None
    for x_ref, c_ref in ((xa_ref, ca_ref), (xb_ref, cb_ref)):
        x, c = x_ref[0], c_ref[0]
        u, dab = act(nn(x, w13_ref[0]), nt(c, w2_ref[0]))
        p13, p2 = tn(x, dab), tn(u, c)
        d13, d2 = (p13, p2) if d13 is None else (d13 + p13, d2 + p2)
    if accumulate:
        g1_ref[0] = refs[0][0] + d13[:, :ff]
        g3_ref[0] = refs[1][0] + d13[:, ff:]
        g2_ref[0] = refs[2][0] + d2
    else:
        g1_ref[0] = d13[:, :ff]
        g3_ref[0] = d13[:, ff:]
        g2_ref[0] = d2


def row_kernel(slots, xa_ref, xb_ref, ca_ref, cb_ref, wo_ref, w2o_ref, wp_ref, w2p_ref, *r_refs):
    for q, (x_ref, c_ref) in enumerate(((xa_ref, ca_ref), (xb_ref, cb_ref))):
        x, c = x_ref[0], c_ref[0]
        y, dx = None, None
        for w_ref, v_ref in ((wo_ref, w2o_ref), (wp_ref, w2p_ref)):
            u, dab = act(nn(x, w_ref[0]), nt(c, v_ref[0]))
            py, pdx = nn(u, v_ref[0]), nt(dab, w_ref[0])
            y, dx = (py, pdx) if y is None else (y + py, dx + pdx)
        y, dx = y.astype(bf16), dx.astype(bf16)
        for b in range(2):
            r_refs[2 * q + b][0, 0] = y[b * slots:(b + 1) * slots]
            r_refs[2 * q + b][0, 1] = dx[b * slots:(b + 1) * slots]


def combine_kernel(groups, accumulate, slots, n_local, info_ref, code_ref, *refs):
    n_r = 4 * len(groups)
    r_refs, rest = refs[:n_r], refs[n_r:]
    y0_ref, y1_ref, dx_ref = rest[-3:]
    code = code_ref[...]
    e0, e1, pos0, pos1 = (code[:, k:k + 1].astype(jnp.int32) for k in range(4))
    rows = code.shape[0]
    lane = iota((rows, slots), 1)
    y, dx = None, None
    for gi, (lo, hi) in enumerate(groups):
        for q in range(4):
            r_ref = r_refs[4 * gi + q]
            for el in range(hi - lo):
                expert = info_ref[q] * n_local + lo + el
                one = lambda e, pos: jnp.where(lane == jnp.where(e == expert, pos, -1), 1.0, 0.0)
                m0, m1 = one(e0, pos0), one(e1, pos1)
                py = nn(jnp.concatenate([m0, m1], axis=0).astype(bf16), r_ref[el, 0])
                pdx = nn((m0 + m1).astype(bf16), r_ref[el, 1])
                y, dx = (py, pdx) if y is None else (y + py, dx + pdx)
    if accumulate:
        y0_ref[...] = (rest[0][...].astype(f32) + y[:rows]).astype(bf16)
        y1_ref[...] = (rest[1][...].astype(f32) + y[rows:]).astype(bf16)
        dx_ref[...] = rest[2][...] + dx
    else:
        y0_ref[...] = y[:rows].astype(bf16)
        y1_ref[...] = y[rows:].astype(bf16)
        dx_ref[...] = dx


def final_kernel(h_ref, d_ref, y0_ref, y1_ref, dx_ref, code_ref, p_ref, coef_ref, wr_ref, stat_ref,
                 out_ref, dh_ref, dr_ref):
    n_experts = p_ref.shape[1]
    code, p = code_ref[...], p_ref[...]
    e0, e1 = code[:, 0:1].astype(jnp.int32), code[:, 1:2].astype(jnp.int32)
    g0, g1, s = code[:, 4:5], code[:, 5:6], code[:, 6:7]
    h = h_ref[...]
    d = d_ref[...].astype(f32)
    y0, y1 = y0_ref[...].astype(f32), y1_ref[...].astype(f32)
    out_ref[...] = (h.astype(f32) + OUT_SCALE * (g0 * y0 + g1 * y1)).astype(bf16)
    m = OUT_SCALE * d
    dg0 = jnp.sum(m * y0, axis=1, keepdims=True)
    dg1 = jnp.sum(m * y1, axis=1, keepdims=True)
    mean = g0 * dg0 + g1 * dg1
    lane = iota(p.shape, 1)
    dp = (jnp.where(lane == e0, (dg0 - mean) / s, 0.0) + jnp.where(lane == e1, (dg1 - mean) / s, 0.0)
          + coef_ref[...])
    dz = p * (dp - jnp.sum(p * dp, axis=1, keepdims=True))
    z3 = split3(dz)
    w_hi, w_lo, _ = split3(wr_ref[...])
    back = nt(z3[0], w_hi) + (nt(z3[1], w_hi) + nt(z3[0], w_lo))
    dh_ref[...] = (d + dx_ref[...] + back).astype(bf16)
    part = tn(z3[0], h) + (tn(z3[1], h) + tn(z3[2], h))

    @pl.when(pl.program_id(0) == 0)
    def _():
        dr_ref[...] = jnp.zeros_like(dr_ref)
        dr_ref[n_experts:n_experts + 1, 0:n_experts] = stat_ref[1:2, 0:n_experts]

    dr_ref[0:n_experts, :] = dr_ref[0:n_experts, :] + part


def solution(mesh):
    ep_size = mesh.shape["ep"]
    etp_size = mesh.shape["etp"]
    n_dev = ep_size * etp_size
    all_axes = ("ep", "etp")
    tok_spec = P(all_axes, None)
    gate_spec = P("ep", None, "etp")
    down_spec = P("ep", "etp", None)

    def permute(v, dep, detp):
        pairs = [(t * ep_size + o, (t ^ detp) * ep_size + (o ^ dep)) for t in range(etp_size) for o in range(ep_size)]
        return lax.ppermute(v, ("etp", "ep"), pairs)

    def layer(hidden, w_router, expert_ids, d_out, w_gate, w_up, w_down):
        tok_rows, d_model = hidden.shape
        n_experts = w_router.shape[1]
        n_local, _, ff = w_gate.shape
        n_tokens = tok_rows * n_dev
        capacity = (5 * n_tokens + 2 * n_experts - 1) // (2 * n_experts)
        slots = 7 * tok_rows // (2 * n_experts)
        ep, etp = lax.axis_index("ep"), lax.axis_index("etp")
        steps = tok_rows // TILE
        sds = jax.ShapeDtypeStruct
        smem = pl.BlockSpec(memory_space=pltpu.SMEM)

        def whole(shape):
            return pl.BlockSpec(shape, lambda i: (0,) * len(shape))

        def tokens(width, tile=TILE):
            return pl.BlockSpec((tile, width), lambda i: (i, 0))

        def expert_block(shape, lo=0):
            return pl.BlockSpec((1,) + shape, lambda i: (i + lo,) + (0,) * len(shape))

        hx, hy = permute(hidden, 2, 0), permute(hidden, 0, 1)

        probs, code, pay = pl.pallas_call(
            functools.partial(route_kernel, n_experts),
            grid=(steps,),
            in_specs=[tokens(d_model), whole((d_model, n_experts)), tokens(2)],
            out_specs=[tokens(n_experts), tokens(128), whole((PAY_T + 8 * steps, TILE))],
            out_shape=[sds((tok_rows, n_experts), f32), sds((tok_rows, 128), f32), sds((PAY_T + 8 * steps, TILE), f32)],
            compiler_params=params(), cost_estimate=cost(3e9), name="route",
        )(hidden, w_router, expert_ids)
        pays = lax.all_gather(pay, all_axes)
        counts = pays[:, n_experts, :n_experts]
        total = jnp.sum(counts, axis=0, keepdims=True)
        coef = (AUX_COEF * n_experts / n_tokens / (2 * n_tokens)) * total

        w13 = jnp.concatenate([w_gate, w_up], axis=2)
        d_send, w13_send, w2_send, pays = lax.optimization_barrier((d_out, w13, w_down, pays))
        dx_, dy_ = permute(d_send, 2, 0), permute(d_send, 0, 1)
        hd, dd = permute(hy, 2, 0), permute(dy_, 2, 0)
        core = lambda v: permute(v, 1, 0)
        h_pairs = {(0, 0): (hidden, core(hidden)), (1, 0): (hx, core(hx)), (0, 1): (hy, core(hy)), (1, 1): (hd, core(hd))}
        d_pairs = {(0, 0): (d_out, core(d_out)), (1, 0): (dx_, core(dx_)), (0, 1): (dy_, core(dy_)), (1, 1): (dd, core(dd))}
        partner = [(permute(w13_send[lo:hi], 0, 1), permute(w2_send[lo:hi], 0, 1)) for lo, hi in CHUNKS]

        def gather(pair):
            x, t = pair
            info = jnp.stack([(ep ^ (2 * x)) * etp_size + (etp ^ t), (ep ^ (2 * x + 1)) * etp_size + (etp ^ t), ep * n_local]).astype(jnp.int32)
            block = sds((n_local, 2 * slots, d_model), bf16)
            return pl.pallas_call(
                functools.partial(gather_kernel, capacity, slots),
                grid=(n_local,),
                in_specs=[smem, whole((n_dev, n_experts)), whole(pays.shape)] + [whole((tok_rows, d_model))] * 4,
                out_specs=[expert_block((2 * slots, d_model))] * 2,
                out_shape=[block, block],
                scratch_shapes=[pltpu.VMEM((slots, tok_rows), bf16)],
                compiler_params=params(), cost_estimate=cost(15e9), name=f"gather{x}{t}",
            )(info, counts, pays, *h_pairs[pair], *d_pairs[pair])

        rows = {pair: gather(pair) for pair in h_pairs}
        row_block = expert_block((2 * slots, d_model))
        g13, g2 = expert_block((d_model, ff)), expert_block((ff, d_model))

        def grads(first, second, acc):
            (xa, ca), (xb, cb) = rows[first], rows[second]
            return pl.pallas_call(
                functools.partial(grad_kernel, bool(acc)),
                grid=(n_local,),
                in_specs=[row_block] * 4 + [expert_block((d_model, 2 * ff)), expert_block((ff, d_model))] + [g13, g13, g2][:len(acc)],
                out_specs=[g13, g13, g2],
                out_shape=[sds((n_local, d_model, ff), f32)] * 2 + [sds((n_local, ff, d_model), f32)],
                input_output_aliases={6 + k: k for k in range(len(acc))},
                compiler_params=params(), cost_estimate=cost(25e9), name=f"grads{len(acc)}",
            )(xa, xb, ca, cb, w13, w_down, *acc)

        grad = grads((0, 0), (1, 0), ())
        g_gate, g_up, g_down = grads((0, 1), (1, 1), tuple(grad))

        def back(index):
            lo, hi = CHUNKS[index]
            (xa, ca), (xb, cb) = rows[(0, 0)], rows[(1, 0)]
            at = lambda shape: expert_block(shape, lo)
            outs = pl.pallas_call(
                functools.partial(row_kernel, slots),
                grid=(hi - lo,),
                in_specs=[at((2 * slots, d_model))] * 4 + [at((d_model, 2 * ff)), at((ff, d_model)),
                          expert_block((d_model, 2 * ff)), expert_block((ff, d_model))],
                out_specs=[expert_block((2, slots, d_model))] * 4,
                out_shape=[sds((hi - lo, 2, slots, d_model), bf16)] * 4,
                compiler_params=params(), cost_estimate=cost(6e9 * (hi - lo)), name=f"rows{index}",
            )(xa, xb, ca, cb, w13, w_down, *partner[index])
            return [outs[0]] + [permute(outs[q], q, 0) for q in (1, 2, 3)]

        returned = [back(i) for i in range(len(CHUNKS))]
        ep_info = jnp.stack([ep ^ q for q in range(4)]).astype(jnp.int32)

        def combine(chunk_ids, acc):
            groups = tuple(CHUNKS[i] for i in chunk_ids)
            arrays = [r for i in chunk_ids for r in returned[i]]
            tile = 512
            acc_specs = [tokens(d_model, tile)] * 3
            return pl.pallas_call(
                functools.partial(combine_kernel, groups, bool(acc), slots, n_local),
                grid=(tok_rows // tile,),
                in_specs=[smem, tokens(128, tile)] + [whole(r.shape) for r in arrays] + acc_specs[:len(acc)],
                out_specs=acc_specs,
                out_shape=[sds((tok_rows, d_model), bf16)] * 2 + [sds((tok_rows, d_model), f32)],
                compiler_params=params(), cost_estimate=cost(14e9 * len(chunk_ids)), name=f"combine{chunk_ids[0]}",
            )(ep_info, code, *arrays, *acc)

        acc = combine((0, 1, 2), ())
        y0, y1, dxs = combine((3,), tuple(acc))

        output, d_hidden, d_rt = pl.pallas_call(
            final_kernel,
            grid=(steps,),
            in_specs=[tokens(d_model)] * 5 + [tokens(128), tokens(n_experts), whole((1, n_experts)), whole((d_model, n_experts)),
                      pl.BlockSpec((8, TILE), lambda i: (n_experts // 8, 0))],
            out_specs=[tokens(d_model)] * 2 + [whole((n_experts + 8, d_model))],
            out_shape=[sds((tok_rows, d_model), bf16)] * 2 + [sds((n_experts + 8, d_model), f32)],
            compiler_params=params(), cost_estimate=cost(4e9), name="final",
        )(hidden, d_out, y0, y1, dxs, code, probs, coef, w_router, pay)
        d_rt = lax.psum(d_rt, all_axes)
        d_router = d_rt[:n_experts].T
        route_frac = total[0] / (2 * n_tokens)
        aux_loss = AUX_COEF * n_experts * jnp.sum(route_frac * (d_rt[n_experts, :n_experts] / n_tokens))
        return output, d_hidden, d_router, aux_loss, g_gate, g_up, g_down

    return jax.shard_map(layer, mesh=mesh, in_specs=(tok_spec, P(), tok_spec, tok_spec, gate_spec, gate_spec, down_spec), out_specs=(tok_spec, tok_spec, P(), P(), gate_spec, gate_spec, down_spec), check_vma=False)
```

```python
import functools
import jax
import jax.numpy as jnp
from jax import lax
from jax.experimental import pallas as pl
from jax.experimental.pallas import tpu as pltpu
from jax.sharding import PartitionSpec as P

AUX_COEF = 0.01
OUT_SCALE = 2.0
CHUNKS = ((0, 2), (2, 4), (4, 6), (6, 7), (7, 8))

f32, bf16 = jnp.float32, jnp.bfloat16
TILE = 256
WIN = 48


def nn(a, b):
    return jnp.dot(a, b, preferred_element_type=f32)


def nt(a, b):
    return lax.dot_general(a, b, (((1,), (1,)), ((), ())), preferred_element_type=f32)


def tn(a, b):
    return lax.dot_general(a, b, (((0,), (0,)), ((), ())), preferred_element_type=f32)


def split3(v):
    hi = v.astype(bf16)
    rest = v - hi.astype(f32)
    mid = rest.astype(bf16)
    return hi, mid, (rest - mid.astype(f32)).astype(bf16)


def iota(shape, dim):
    return lax.broadcasted_iota(jnp.int32, shape, dim)


def params(**kw):
    return pltpu.CompilerParams(vmem_limit_bytes=60 * 2**20, **kw)


def cost(flops):
    return pl.CostEstimate(flops=int(flops), bytes_accessed=1 << 20, transcendentals=0)


def route_kernel(n_experts, h_ref, wr_ref, ids_ref, p_ref, code_ref, win_ref, stat_ref):
    step = pl.program_id(0)

    @pl.when(step == 0)
    def _():
        stat_ref[...] = jnp.zeros_like(stat_ref)
        win_ref[...] = jnp.zeros_like(win_ref)

    w_hi, w_mid, w_lo = split3(wr_ref[...])
    h = h_ref[...]
    z = (nn(h, w_lo) + nn(h, w_mid)) + nn(h, w_hi)
    z = jnp.exp(z - jnp.max(z, axis=1, keepdims=True))
    p = z / jnp.sum(z, axis=1, keepdims=True)
    p_ref[...] = p
    ids = ids_ref[...]
    lane = iota((TILE, n_experts), 1)
    e0, e1 = ids[:, 0:1], ids[:, 1:2]
    m0, m1 = lane == e0, lane == e1
    hist = jnp.where(m0 | m1, 1.0, 0.0).astype(f32)
    before = (iota((TILE, TILE), 1) < iota((TILE, TILE), 0)).astype(f32).astype(bf16)
    seen = stat_ref[0:1, 0:n_experts]
    after = seen + jnp.sum(hist, axis=0, keepdims=True)
    start = jnp.floor(seen * (1.0 / 16)) * 16
    n_win = jnp.max(jnp.floor((after - start + (WIN - 1)) * (1.0 / WIN) + 1e-3), axis=1, keepdims=True)
    rank = nn(before, hist.astype(bf16)) + seen
    pick = lambda m, v: jnp.sum(jnp.where(m, v, 0.0), axis=1, keepdims=True)
    p0, p1 = pick(m0, p), pick(m1, p)
    s = p0 + p1
    wide = iota((TILE, 128), 1)
    code = jnp.zeros((TILE, 128), f32)
    rel = rank - start
    for k, v in enumerate((e0.astype(f32), e1.astype(f32), pick(m0, rel), pick(m1, rel), p0 / s, p1 / s, s)):
        code = jnp.where(wide == k, v, code)
    code_ref[...] = code
    win_ref[pl.ds(step, 1), 0:n_experts] = start.astype(jnp.int32)
    win_ref[pl.ds(step, 1), n_experts:n_experts + 1] = n_win.astype(jnp.int32)
    stat_ref[0:1, 0:n_experts] = after
    stat_ref[1:2, 0:n_experts] = stat_ref[1:2, 0:n_experts] + jnp.sum(p, axis=0, keepdims=True)


def slot_kernel(capacity, slots, n_local, info_ref, ids_ref, wr_ref, slot_ref, other_ref, start_ref, wr3_ref, total_ref):
    @pl.when(pl.program_id(0) == 0)
    def _():
        total_ref[...] = jnp.zeros_like(total_ref)
        wr3_ref[...] = jnp.zeros_like(wr3_ref)
        width = wr_ref.shape[1]
        for k, piece in enumerate(split3(wr_ref[...])):
            wr3_ref[:, k * width:(k + 1) * width] = piece

    steps = ids_ref.shape[1] // 2
    expert = iota((n_local, TILE), 0) + info_ref[0]
    before = (iota((TILE, TILE), 0) < iota((TILE, TILE), 1)).astype(f32).astype(bf16)
    row = iota((TILE, TILE), 0).astype(f32)
    lane = iota((n_local, 128), 1)
    carry = jnp.zeros((n_local, 1), f32)
    starts = jnp.zeros((n_local, 128), f32)
    other = jnp.zeros((n_local, TILE), f32)
    for i in range(steps):
        e0, e1 = ids_ref[0, 2 * i:2 * i + 1, :], ids_ref[0, 2 * i + 1:2 * i + 2, :]
        m0, m1 = expert == e0, expert == e1
        hit = jnp.where(m0 | m1, 1.0, 0.0).astype(f32)
        rank = nn(hit.astype(bf16), before) + carry
        slot_ref[0, i * n_local:(i + 1) * n_local, :] = jnp.where(m0 | m1, rank, -1.0)
        starts = jnp.where(lane == i, carry, starts)
        for m, e in ((m0, e1), (m1, e0)):
            pos = jnp.sum(jnp.where(m, rank + 1.0, 0.0), axis=0, keepdims=True) - 1.0
            one = jnp.where(row == pos, 1.0, 0.0).astype(bf16)
            other = other + nt(jnp.where(m, e.astype(f32), 0.0).astype(bf16), one)
        carry = carry + jnp.sum(hit, axis=1, keepdims=True)
    other_ref[0] = other
    prefix = total_ref[:, 0:1]
    room = jnp.clip(capacity - prefix, 0.0, float(slots))
    starts = jnp.where(lane == steps, carry, jnp.where(lane == steps + 1, jnp.minimum(room, carry), starts))
    start_ref[0] = starts.astype(jnp.int32)
    total_ref[...] = total_ref[...] + carry


def gather_kernel(slots, n_local, n_experts, info_ref, start_ref, slot_ref, other_ref, wr3_ref, ha_ref, hb_ref, da_ref, db_ref,
                  x_ref, c_ref, m_ref, xs_ref, ds_ref):
    step = pl.program_id(0)
    steps = pl.num_programs(0) - n_local

    @pl.when(step < steps)
    def _():
        row = iota((WIN, TILE), 0)
        for b, (h_ref, d_ref) in enumerate(((ha_ref, da_ref), (hb_ref, db_ref))):
            j = info_ref[b]
            first = [(start_ref[j, e, step] // 16) * 16 for e in range(n_local)]
            span = functools.reduce(jnp.maximum, [start_ref[j, e, step + 1] - first[e] for e in range(n_local)])

            def window(w, carry):
                for e in range(n_local):
                    slot = slot_ref[j, pl.ds(step * n_local + e, 1), :]
                    hit = (row + (first[e] + w * WIN)).astype(f32) == slot
                    m_ref[e * WIN:(e + 1) * WIN, :] = jnp.where(hit, 1.0, 0.0).astype(bf16)
                m = m_ref[...]
                for src, dst in ((h_ref, xs_ref), (d_ref, ds_ref)):
                    r = nn(m, src[...]).astype(bf16)
                    for e in range(n_local):
                        at = pl.multiple_of(jnp.minimum(first[e] + w * WIN, slots + 16), 16)
                        old = dst[b, e, pl.ds(at, 16), :]
                        keep = iota((16, 1), 0) + at < start_ref[j, e, step]
                        head = r[e * WIN:e * WIN + 16].astype(f32)
                        dst[b, e, pl.ds(at, 16), :] = jnp.where(keep, old.astype(f32), head).astype(bf16)
                        dst[b, e, pl.ds(pl.multiple_of(at + 16, 16), WIN - 16), :] = r[e * WIN + 16:(e + 1) * WIN]
                return carry

            lax.fori_loop(0, (span + WIN - 1) // WIN, window, 0)

    @pl.when(step >= steps)
    def _():
        e = step - steps
        lane = iota((slots, 128), 1)
        for b in range(2):
            j = info_ref[b]
            kept = iota((slots, 1), 0) < start_ref[j, e, steps + 1]
            x = jnp.where(kept, xs_ref[b, e, 0:slots, :].astype(f32), 0.0)
            d = jnp.where(kept, ds_ref[b, e, 0:slots, :].astype(f32), 0.0)
            x = x.astype(bf16)
            x_ref[0, b * slots:(b + 1) * slots, :] = x
            z = nn(x, wr3_ref[...])
            other = other_ref[j].T[0:slots, :]
            other = jnp.sum(jnp.where(iota((slots, n_local), 1) == e, other, 0.0), axis=1, keepdims=True)
            name = lane % n_experts
            here = jnp.sum(jnp.where(name == info_ref[2] + e, z, 0.0), axis=1, keepdims=True)
            there = jnp.sum(jnp.where(name == other.astype(jnp.int32), z, 0.0), axis=1, keepdims=True)
            g = 1.0 / (1.0 + jnp.exp(there - here))
            c_ref[0, b * slots:(b + 1) * slots, :] = (g * (OUT_SCALE * d)).astype(bf16)


def act(ab, du):
    ff = du.shape[1]
    a, b = ab[:, :ff], ab[:, ff:]
    sig = jax.nn.sigmoid(a)
    silu = a * sig
    u = (silu * b).astype(bf16)
    da = (du * b * sig * (1.0 + a * (1.0 - sig))).astype(bf16)
    db = (du * silu).astype(bf16)
    return u, jnp.concatenate([da, db], axis=1)


def grad_kernel(accumulate, xa_ref, xb_ref, ca_ref, cb_ref, w13_ref, w2_ref, *refs):
    g1_ref, g3_ref, g2_ref = refs[-3:]
    ff = w2_ref.shape[1]
    d13, d2 = None, None
    for x_ref, c_ref in ((xa_ref, ca_ref), (xb_ref, cb_ref)):
        x, c = x_ref[0], c_ref[0]
        u, dab = act(nn(x, w13_ref[0]), nt(c, w2_ref[0]))
        p13, p2 = tn(x, dab), tn(u, c)
        d13, d2 = (p13, p2) if d13 is None else (d13 + p13, d2 + p2)
    if accumulate:
        g1_ref[0] = refs[0][0] + d13[:, :ff]
        g3_ref[0] = refs[1][0] + d13[:, ff:]
        g2_ref[0] = refs[2][0] + d2
    else:
        g1_ref[0] = d13[:, :ff]
        g3_ref[0] = d13[:, ff:]
        g2_ref[0] = d2


def row_kernel(slots, xa_ref, xb_ref, ca_ref, cb_ref, wo_ref, w2o_ref, wp_ref, w2p_ref, *r_refs):
    for q, (x_ref, c_ref) in enumerate(((xa_ref, ca_ref), (xb_ref, cb_ref))):
        x, c = x_ref[0], c_ref[0]
        y, dx = None, None
        for w_ref, v_ref in ((wo_ref, w2o_ref), (wp_ref, w2p_ref)):
            u, dab = act(nn(x, w_ref[0]), nt(c, v_ref[0]))
            py, pdx = nn(u, v_ref[0]), nt(dab, w_ref[0])
            y, dx = (py, pdx) if y is None else (y + py, dx + pdx)
        y, dx = y.astype(bf16), dx.astype(bf16)
        for b in range(2):
            r_refs[2 * q + b][0, 0] = y[b * slots:(b + 1) * slots]
            r_refs[2 * q + b][0, 1] = dx[b * slots:(b + 1) * slots]


def combine_kernel(groups, accumulate, slots, n_local, info_ref, win_ref, code_ref, *refs):
    n_r = 4 * len(groups)
    r_refs, rest = refs[:n_r], refs[n_r:-2]
    y0_ref, y1_ref, dx_ref = rest[-3:]
    yc_ref, xc_ref = refs[-2:]
    step = pl.program_id(0)
    code = code_ref[...]
    rows = code.shape[0]
    n_experts = 4 * n_local
    names = [(q, lo + el, r_refs[4 * gi + q], el) for gi, (lo, hi) in enumerate(groups) for q in range(4) for el in range(hi - lo)]
    width = len(names) * WIN
    lane = iota((rows, width), 1)
    place = []
    for k in range(2):
        e = code[:, k:k + 1].astype(jnp.int32)
        q, el = (e // n_local) ^ info_ref[0], e % n_local
        index = jnp.full(e.shape, -(1 << 20), jnp.int32)
        done = 0
        for lo, hi in groups:
            index = jnp.where((el >= lo) & (el < hi), done + q * (hi - lo) + (el - lo), index)
            done += 4 * (hi - lo)
        place.append(index * WIN)
    rel = [code[:, k:k + 1].astype(jnp.int32) for k in (2, 3)]

    def window(w, acc):
        y, dx = acc
        for i, (q, el_abs, r_ref, el) in enumerate(names):
            first = win_ref[step, info_ref[q] * n_local + el_abs]
            for piece in range(0, WIN, 16):
                at = pl.multiple_of(jnp.minimum(first + w * WIN + piece, slots - 16), 16)
                yc_ref[i * WIN + piece:i * WIN + piece + 16, :] = r_ref[el, 0, pl.ds(at, 16), :]
                xc_ref[i * WIN + piece:i * WIN + piece + 16, :] = r_ref[el, 1, pl.ds(at, 16), :]
        ms = []
        for k in range(2):
            inside = (rel[k] >= w * WIN) & (rel[k] < w * WIN + WIN)
            at = jnp.where(inside, place[k] + rel[k] - w * WIN, -1)
            ms.append(jnp.where(lane == at, 1.0, 0.0))
        m0, m1 = ms
        y = y + nn(jnp.concatenate([m0, m1], axis=0).astype(bf16), yc_ref[...])
        dx = dx + nn((m0 + m1).astype(bf16), xc_ref[...])
        return y, dx

    d_model = y0_ref.shape[1]
    y, dx = window(0, (jnp.zeros((2 * rows, d_model), f32), jnp.zeros((rows, d_model), f32)))
    if accumulate:
        y0_ref[...] = (rest[0][...].astype(f32) + y[:rows]).astype(bf16)
        y1_ref[...] = (rest[1][...].astype(f32) + y[rows:]).astype(bf16)
        dx_ref[...] = rest[2][...] + dx
    else:
        y0_ref[...] = y[:rows].astype(bf16)
        y1_ref[...] = y[rows:].astype(bf16)
        dx_ref[...] = dx
    n_win = win_ref[step, n_experts]

    @pl.when(n_win > 1)
    def _():
        def more(w, carry):
            y, dx = window(w, (jnp.zeros((2 * rows, d_model), f32), jnp.zeros((rows, d_model), f32)))
            y0_ref[...] = (y0_ref[...].astype(f32) + y[:rows]).astype(bf16)
            y1_ref[...] = (y1_ref[...].astype(f32) + y[rows:]).astype(bf16)
            dx_ref[...] = dx_ref[...] + dx
            return carry

        lax.fori_loop(1, n_win, more, 0)


def final_kernel(h_ref, d_ref, y0_ref, y1_ref, dx_ref, code_ref, p_ref, coef_ref, wr_ref, stat_ref,
                 out_ref, dh_ref, dr_ref):
    n_experts = p_ref.shape[1]
    code, p = code_ref[...], p_ref[...]
    e0, e1 = code[:, 0:1].astype(jnp.int32), code[:, 1:2].astype(jnp.int32)
    g0, g1, s = code[:, 4:5], code[:, 5:6], code[:, 6:7]
    h = h_ref[...]
    d = d_ref[...].astype(f32)
    y0, y1 = y0_ref[...].astype(f32), y1_ref[...].astype(f32)
    out_ref[...] = (h.astype(f32) + OUT_SCALE * (g0 * y0 + g1 * y1)).astype(bf16)
    m = OUT_SCALE * d
    dg0 = jnp.sum(m * y0, axis=1, keepdims=True)
    dg1 = jnp.sum(m * y1, axis=1, keepdims=True)
    mean = g0 * dg0 + g1 * dg1
    lane = iota(p.shape, 1)
    dp = (jnp.where(lane == e0, (dg0 - mean) / s, 0.0) + jnp.where(lane == e1, (dg1 - mean) / s, 0.0)
          + coef_ref[...])
    dz = p * (dp - jnp.sum(p * dp, axis=1, keepdims=True))
    z3 = split3(dz)
    w_hi, w_lo, _ = split3(wr_ref[...])
    back = nt(z3[0], w_hi) + (nt(z3[1], w_hi) + nt(z3[0], w_lo))
    dh_ref[...] = (d + dx_ref[...] + back).astype(bf16)
    part = tn(z3[0], h) + (tn(z3[1], h) + tn(z3[2], h))

    @pl.when(pl.program_id(0) == 0)
    def _():
        dr_ref[...] = jnp.zeros_like(dr_ref)
        dr_ref[n_experts:n_experts + 1, 0:128] = stat_ref[1:2, :]

    dr_ref[0:n_experts, :] = dr_ref[0:n_experts, :] + part


def solution(mesh):
    ep_size = mesh.shape["ep"]
    etp_size = mesh.shape["etp"]
    n_dev = ep_size * etp_size
    all_axes = ("ep", "etp")
    tok_spec = P(all_axes, None)
    gate_spec = P("ep", None, "etp")
    down_spec = P("ep", "etp", None)

    def permute(v, dep, detp):
        pairs = [(t * ep_size + o, (t ^ detp) * ep_size + (o ^ dep)) for t in range(etp_size) for o in range(ep_size)]
        return lax.ppermute(v, ("etp", "ep"), pairs)

    def kernel(body, **kw):
        return pl.pallas_call(body, **kw)

    def layer(hidden, w_router, expert_ids, d_out, w_gate, w_up, w_down):
        tok_rows, d_model = hidden.shape
        n_experts = w_router.shape[1]
        n_local, _, ff = w_gate.shape
        n_tokens = tok_rows * n_dev
        capacity = (5 * n_tokens + 2 * n_experts - 1) // (2 * n_experts)
        slots = 7 * tok_rows // (2 * n_experts)
        ep, etp = lax.axis_index("ep"), lax.axis_index("etp")
        steps = tok_rows // TILE
        sds = jax.ShapeDtypeStruct
        smem = pl.BlockSpec(memory_space=pltpu.SMEM)

        def whole(shape):
            return pl.BlockSpec(shape, lambda i: (0,) * len(shape))

        def tokens(width, tile=TILE):
            return pl.BlockSpec((tile, width), lambda i: (i, 0))

        def expert_block(shape, lo=0):
            return pl.BlockSpec((1,) + shape, lambda i: (i + lo,) + (0,) * len(shape))

        tile_ids = expert_ids.reshape(steps, TILE, 2).transpose(0, 2, 1).reshape(2 * steps, TILE)
        all_ids = lax.all_gather(tile_ids, all_axes)
        w13 = jnp.concatenate([w_gate, w_up], axis=2)
        h_send, d_send, w13_send, w2_send, all_ids = lax.optimization_barrier((hidden, d_out, w13, w_down, all_ids))

        hx, hy = permute(h_send, 2, 0), permute(h_send, 0, 1)
        dx_, dy_ = permute(d_send, 2, 0), permute(d_send, 0, 1)
        hd, dd = permute(hy, 2, 0), permute(dy_, 2, 0)
        core = lambda v: permute(v, 1, 0)
        h_pairs = {(0, 0): (hidden, core(h_send)), (1, 0): (hx, core(hx)), (0, 1): (hy, core(hy)), (1, 1): (hd, core(hd))}
        d_pairs = {(0, 0): (d_out, core(d_send)), (1, 0): (dx_, core(dx_)), (0, 1): (dy_, core(dy_)), (1, 1): (dd, core(dd))}
        partner = [(permute(w13_send[lo:hi], 0, 1), permute(w2_send[lo:hi], 0, 1)) for lo, hi in CHUNKS]

        per_block = lambda *shape: pl.BlockSpec((1,) + shape, lambda i: (i,) + (0,) * len(shape))
        slot_rows, others, starts, wr3 = kernel(
            functools.partial(slot_kernel, capacity, slots, n_local),
            grid=(n_dev,),
            in_specs=[smem, per_block(2 * steps, TILE), whole((d_model, n_experts))],
            out_specs=[per_block(steps * n_local, TILE), per_block(n_local, TILE), per_block(n_local, 128), whole((d_model, 128))],
            out_shape=[sds((n_dev, steps * n_local, TILE), f32), sds((n_dev, n_local, TILE), f32),
                       sds((n_dev, n_local, 128), jnp.int32), sds((d_model, 128), bf16)],
            scratch_shapes=[pltpu.VMEM((n_local, 128), f32)],
            compiler_params=params(), cost_estimate=cost(5e9),
        )((ep * n_local).astype(jnp.int32)[None], all_ids, w_router)

        probs, code, wins, stats = kernel(
            functools.partial(route_kernel, n_experts),
            grid=(steps,),
            in_specs=[tokens(d_model), whole((d_model, n_experts)), tokens(2)],
            out_specs=[tokens(n_experts), tokens(128), whole((8, 128)), whole((8, 128))],
            out_shape=[sds((tok_rows, n_experts), f32), sds((tok_rows, 128), f32), sds((8, 128), jnp.int32), sds((8, 128), f32)],
            compiler_params=params(), cost_estimate=cost(3e9),
        )(hidden, w_router, expert_ids)

        def gather(pair):
            x, t = pair
            info = jnp.stack([(ep ^ (2 * x)) * etp_size + (etp ^ t), (ep ^ (2 * x + 1)) * etp_size + (etp ^ t), ep * n_local]).astype(jnp.int32)
            block = sds((n_local, 2 * slots, d_model), bf16)
            tile = pl.BlockSpec((TILE, d_model), lambda i: (jnp.minimum(i, steps - 1), 0))
            out = pl.BlockSpec((1, 2 * slots, d_model), lambda i: (jnp.maximum(i - steps, 0), 0, 0))
            return kernel(
                functools.partial(gather_kernel, slots, n_local, n_experts),
                grid=(steps + n_local,),
                in_specs=[smem, smem, whole(slot_rows.shape), whole(others.shape), whole(wr3.shape)] + [tile] * 4,
                out_specs=[out] * 2,
                out_shape=[block, block],
                scratch_shapes=[pltpu.VMEM((n_local * WIN, TILE), bf16)] + [pltpu.VMEM((2, n_local, slots + 64, d_model), bf16)] * 2,
                compiler_params=params(), cost_estimate=cost(8e9),
            )(info, starts, slot_rows, others, wr3, *h_pairs[pair], *d_pairs[pair])

        rows = {pair: gather(pair) for pair in h_pairs}
        row_block = expert_block((2 * slots, d_model))
        g13, g2 = expert_block((d_model, ff)), expert_block((ff, d_model))

        def grads(first, second, acc):
            (xa, ca), (xb, cb) = rows[first], rows[second]
            return kernel(
                functools.partial(grad_kernel, bool(acc)),
                grid=(n_local,),
                in_specs=[row_block] * 4 + [expert_block((d_model, 2 * ff)), expert_block((ff, d_model))] + [g13, g13, g2][:len(acc)],
                out_specs=[g13, g13, g2],
                out_shape=[sds((n_local, d_model, ff), f32)] * 2 + [sds((n_local, ff, d_model), f32)],
                input_output_aliases={6 + k: k for k in range(len(acc))},
                compiler_params=params(), cost_estimate=cost(25e9),
            )(xa, xb, ca, cb, w13, w_down, *acc)

        grad = grads((0, 0), (1, 0), ())
        g_gate, g_up, g_down = grads((0, 1), (1, 1), tuple(grad))

        def back(index):
            lo, hi = CHUNKS[index]
            (xa, ca), (xb, cb) = rows[(0, 0)], rows[(1, 0)]
            at = lambda shape: expert_block(shape, lo)
            outs = kernel(
                functools.partial(row_kernel, slots),
                grid=(hi - lo,),
                in_specs=[at((2 * slots, d_model))] * 4 + [at((d_model, 2 * ff)), at((ff, d_model)),
                          expert_block((d_model, 2 * ff)), expert_block((ff, d_model))],
                out_specs=[expert_block((2, slots, d_model))] * 4,
                out_shape=[sds((hi - lo, 2, slots, d_model), bf16)] * 4,
                compiler_params=params(), cost_estimate=cost(6e9 * (hi - lo)),
            )(xa, xb, ca, cb, w13, w_down, *partner[index])
            return [outs[0]] + [permute(outs[q], q, 0) for q in (1, 2, 3)]

        returned = [back(i) for i in range(len(CHUNKS))]
        total = jnp.sum((all_ids.reshape(-1)[:, None] == jnp.arange(n_experts)[None, :]).astype(f32), axis=0)[None, :]
        coef = (AUX_COEF * n_experts / n_tokens / (2 * n_tokens)) * total
        ep_info = jnp.stack([ep ^ q for q in range(4)]).astype(jnp.int32)

        def combine(chunk_ids, acc):
            groups = tuple(CHUNKS[i] for i in chunk_ids)
            arrays = [r for i in chunk_ids for r in returned[i]]
            acc_specs = [tokens(d_model)] * 3
            width = 4 * sum(hi - lo for lo, hi in groups) * WIN
            return kernel(
                functools.partial(combine_kernel, groups, bool(acc), slots, n_local),
                grid=(steps,),
                in_specs=[smem, smem, tokens(128)] + [whole(r.shape) for r in arrays] + acc_specs[:len(acc)],
                out_specs=acc_specs,
                out_shape=[sds((tok_rows, d_model), bf16)] * 2 + [sds((tok_rows, d_model), f32)],
                scratch_shapes=[pltpu.VMEM((width, d_model), bf16)] * 2,
                compiler_params=params(), cost_estimate=cost(3e9 * len(chunk_ids)),
            )(ep_info, wins, code, *arrays, *acc)

        acc = combine((0, 1), ())
        acc = combine((2, 3), tuple(acc))
        y0, y1, dxs = combine((4,), tuple(acc))

        output, d_hidden, d_rt = kernel(
            final_kernel,
            grid=(steps,),
            in_specs=[tokens(d_model)] * 5 + [tokens(128), tokens(n_experts), whole((1, n_experts)), whole((d_model, n_experts)),
                      whole((8, 128))],
            out_specs=[tokens(d_model)] * 2 + [whole((n_experts + 8, d_model))],
            out_shape=[sds((tok_rows, d_model), bf16)] * 2 + [sds((n_experts + 8, d_model), f32)],
            compiler_params=params(), cost_estimate=cost(4e9),
        )(hidden, d_out, y0, y1, dxs, code, probs, coef, w_router, stats)
        for dep, detp in ((1, 0), (2, 0), (0, 1)):
            d_rt = d_rt + permute(d_rt, dep, detp)
        d_router = d_rt[:n_experts].T
        route_frac = total[0] / (2 * n_tokens)
        aux_loss = AUX_COEF * n_experts * jnp.sum(route_frac * (d_rt[n_experts, :n_experts] / n_tokens))
        return output, d_hidden, d_router, aux_loss, g_gate, g_up, g_down


    return jax.shard_map(layer, mesh=mesh, in_specs=(tok_spec, P(), tok_spec, tok_spec, gate_spec, gate_spec, down_spec), out_specs=(tok_spec, tok_spec, P(), P(), gate_spec, gate_spec, down_spec), check_vma=False)
```

```python
import functools
import jax
import jax.numpy as jnp
from jax import lax
from jax.experimental import pallas as pl
from jax.experimental.pallas import tpu as pltpu
from jax.sharding import PartitionSpec as P

AUX_COEF = 0.01
OUT_SCALE = 2.0
CHUNKS = ((0, 2), (2, 4), (4, 6), (6, 7), (7, 8))

f32, bf16 = jnp.float32, jnp.bfloat16
TILE = 256
WIN = 48


def nn(a, b):
    return jnp.dot(a, b, preferred_element_type=f32)


def nt(a, b):
    return lax.dot_general(a, b, (((1,), (1,)), ((), ())), preferred_element_type=f32)


def tn(a, b):
    return lax.dot_general(a, b, (((0,), (0,)), ((), ())), preferred_element_type=f32)


def split3(v):
    hi = v.astype(bf16)
    rest = v - hi.astype(f32)
    mid = rest.astype(bf16)
    return hi, mid, (rest - mid.astype(f32)).astype(bf16)


def iota(shape, dim):
    return lax.broadcasted_iota(jnp.int32, shape, dim)


def params(**kw):
    return pltpu.CompilerParams(vmem_limit_bytes=60 * 2**20, **kw)


def cost(flops):
    return pl.CostEstimate(flops=int(flops), bytes_accessed=1 << 20, transcendentals=0)


def route_kernel(n_experts, n_local, info_ref, h_ref, wr_ref, ids_ref, p_ref, code_ref, win_ref, stat_ref):
    step = pl.program_id(0)

    @pl.when(step == 0)
    def _():
        stat_ref[...] = jnp.zeros_like(stat_ref)
        win_ref[...] = jnp.zeros_like(win_ref)

    w_hi, w_mid, w_lo = split3(wr_ref[...])
    h = h_ref[...]
    z = (nn(h, w_lo) + nn(h, w_mid)) + nn(h, w_hi)
    z = jnp.exp(z - jnp.max(z, axis=1, keepdims=True))
    p = z / jnp.sum(z, axis=1, keepdims=True)
    p_ref[...] = p
    ids = ids_ref[...]
    lane = iota((TILE, n_experts), 1)
    e0, e1 = ids[:, 0:1], ids[:, 1:2]
    m0, m1 = lane == e0, lane == e1
    hist = jnp.where(m0 | m1, 1.0, 0.0).astype(f32)
    before = (iota((TILE, TILE), 1) < iota((TILE, TILE), 0)).astype(f32).astype(bf16)
    seen = stat_ref[0:1, 0:n_experts]
    after = seen + jnp.sum(hist, axis=0, keepdims=True)
    start = jnp.floor(seen * (1.0 / 16)) * 16
    n_win = jnp.max(jnp.floor((after - start + (WIN - 1)) * (1.0 / WIN) + 1e-3), axis=1, keepdims=True)
    rank = nn(before, hist.astype(bf16)) + seen
    pick = lambda m, v: jnp.sum(jnp.where(m, v, 0.0), axis=1, keepdims=True)
    p0, p1 = pick(m0, p), pick(m1, p)
    s = p0 + p1
    wide = iota((TILE, 128), 1)
    code = jnp.zeros((TILE, 128), f32)
    rel = rank - start
    name = iota((1, n_experts), 1)
    base = ((((name // n_local) ^ info_ref[0]) * n_local + name % n_local) * WIN).astype(f32)
    at = jnp.where(rel < WIN, base + rel, -1.0)
    spread = jnp.zeros_like(rel) + base
    for k, v in enumerate((e0.astype(f32), e1.astype(f32), pick(m0, at), pick(m1, at), p0 / s, p1 / s, s,
                           pick(m0, spread), pick(m1, spread), pick(m0, rel), pick(m1, rel))):
        code = jnp.where(wide == k, v, code)
    code_ref[...] = code
    win_ref[pl.ds(step, 1), 0:n_experts] = start.astype(jnp.int32)
    win_ref[pl.ds(step, 1), 127:128] = n_win.astype(jnp.int32)
    stat_ref[0:1, 0:n_experts] = after
    stat_ref[1:2, 0:n_experts] = stat_ref[1:2, 0:n_experts] + jnp.sum(p, axis=0, keepdims=True)


def slot_kernel(capacity, slots, n_local, info_ref, ids_ref, wr_ref, slot_ref, other_ref, start_ref, wr3_ref, total_ref):
    @pl.when(pl.program_id(0) == 0)
    def _():
        total_ref[...] = jnp.zeros_like(total_ref)
        wr3_ref[...] = jnp.zeros_like(wr3_ref)
        width = wr_ref.shape[1]
        for k, piece in enumerate(split3(wr_ref[...])):
            wr3_ref[:, k * width:(k + 1) * width] = piece

    steps = ids_ref.shape[1] // 2
    near = info_ref[pl.program_id(0)]
    expert = iota((n_local, TILE), 0) + info_ref[info_ref.shape[0] - 1]
    before = (iota((TILE, TILE), 0) < iota((TILE, TILE), 1)).astype(f32).astype(bf16)
    row = iota((TILE, TILE), 0).astype(f32)
    lane = iota((n_local, 128), 1)
    carry = jnp.zeros((n_local, 1), f32)
    starts = jnp.zeros((n_local, 128), f32)
    other = jnp.zeros((n_local, TILE), f32)
    for i in range(steps):
        e0, e1 = ids_ref[near, 2 * i:2 * i + 1, :], ids_ref[near, 2 * i + 1:2 * i + 2, :]
        m0, m1 = expert == e0, expert == e1
        hit = jnp.where(m0 | m1, 1.0, 0.0).astype(f32)
        rank = nn(hit.astype(bf16), before) + carry
        slot_ref[0, i * n_local:(i + 1) * n_local, :] = jnp.where(m0 | m1, rank, -1.0)
        starts = jnp.where(lane == i, carry, starts)
        for m, e in ((m0, e1), (m1, e0)):
            pos = jnp.sum(jnp.where(m, rank + 1.0, 0.0), axis=0, keepdims=True) - 1.0
            one = jnp.where(row == pos, 1.0, 0.0).astype(bf16)
            other = other + nt(jnp.where(m, e.astype(f32), 0.0).astype(bf16), one)
        carry = carry + jnp.sum(hit, axis=1, keepdims=True)
    other_ref[0] = other
    prefix = total_ref[:, 0:1]
    room = jnp.clip(capacity - prefix, 0.0, float(slots))
    starts = jnp.where(lane == steps, carry, jnp.where(lane == steps + 1, jnp.minimum(room, carry), starts))
    start_ref[0] = starts.astype(jnp.int32)
    total_ref[...] = total_ref[...] + carry


def gather_kernel(slots, n_local, n_experts, info_ref, start_ref, slot_ref, other_ref, wr3_ref, ha_ref, hb_ref, da_ref, db_ref,
                  x_ref, c_ref, m_ref, xs_ref, ds_ref):
    step = pl.program_id(0)
    steps = pl.num_programs(0) - n_local

    @pl.when(step < steps)
    def _():
        row = iota((WIN, TILE), 0)
        for b, (h_ref, d_ref) in enumerate(((ha_ref, da_ref), (hb_ref, db_ref))):
            j = info_ref[b]
            first = [(start_ref[j, e, step] // 16) * 16 for e in range(n_local)]
            span = functools.reduce(jnp.maximum, [start_ref[j, e, step + 1] - first[e] for e in range(n_local)])

            def window(w, carry):
                for e in range(n_local):
                    slot = slot_ref[j, pl.ds(step * n_local + e, 1), :]
                    hit = (row + (first[e] + w * WIN)).astype(f32) == slot
                    m_ref[e * WIN:(e + 1) * WIN, :] = jnp.where(hit, 1.0, 0.0).astype(bf16)
                m = m_ref[...]
                for src, dst in ((h_ref, xs_ref), (d_ref, ds_ref)):
                    r = nn(m, src[...]).astype(bf16)
                    for e in range(n_local):
                        at = pl.multiple_of(jnp.minimum(first[e] + w * WIN, slots + 16), 16)
                        old = dst[b, e, pl.ds(at, 16), :]
                        keep = iota((16, 1), 0) + at < start_ref[j, e, step]
                        head = r[e * WIN:e * WIN + 16].astype(f32)
                        dst[b, e, pl.ds(at, 16), :] = jnp.where(keep, old.astype(f32), head).astype(bf16)
                        dst[b, e, pl.ds(pl.multiple_of(at + 16, 16), WIN - 16), :] = r[e * WIN + 16:(e + 1) * WIN]
                return carry

            lax.fori_loop(0, (span + WIN - 1) // WIN, window, 0)

    @pl.when(step >= steps)
    def _():
        e = step - steps
        lane = iota((slots, 128), 1)
        for b in range(2):
            j = info_ref[b]
            kept = iota((slots, 1), 0) < start_ref[j, e, steps + 1]
            x = jnp.where(kept, xs_ref[b, e, 0:slots, :].astype(f32), 0.0)
            d = jnp.where(kept, ds_ref[b, e, 0:slots, :].astype(f32), 0.0)
            x = x.astype(bf16)
            x_ref[0, b * slots:(b + 1) * slots, :] = x
            z = nn(x, wr3_ref[...])
            other = other_ref[j].T[0:slots, :]
            other = jnp.sum(jnp.where(iota((slots, n_local), 1) == e, other, 0.0), axis=1, keepdims=True)
            name = lane % n_experts
            here = jnp.sum(jnp.where(name == info_ref[2] + e, z, 0.0), axis=1, keepdims=True)
            there = jnp.sum(jnp.where(name == other.astype(jnp.int32), z, 0.0), axis=1, keepdims=True)
            g = 1.0 / (1.0 + jnp.exp(there - here))
            c_ref[0, b * slots:(b + 1) * slots, :] = (g * (OUT_SCALE * d)).astype(bf16)


def act(ab, du):
    ff = du.shape[1]
    a, b = ab[:, :ff], ab[:, ff:]
    sig = jax.nn.sigmoid(a)
    silu = a * sig
    u = (silu * b).astype(bf16)
    da = (du * b * sig * (1.0 + a * (1.0 - sig))).astype(bf16)
    db = (du * silu).astype(bf16)
    return u, jnp.concatenate([da, db], axis=1)


def grad_kernel(accumulate, xa_ref, xb_ref, ca_ref, cb_ref, w13_ref, w2_ref, *refs):
    g1_ref, g3_ref, g2_ref = refs[-3:]
    ff = w2_ref.shape[1]
    d13, d2 = None, None
    for x_ref, c_ref in ((xa_ref, ca_ref), (xb_ref, cb_ref)):
        x, c = x_ref[0], c_ref[0]
        u, dab = act(nn(x, w13_ref[0]), nt(c, w2_ref[0]))
        p13, p2 = tn(x, dab), tn(u, c)
        d13, d2 = (p13, p2) if d13 is None else (d13 + p13, d2 + p2)
    if accumulate:
        g1_ref[0] = refs[0][0] + d13[:, :ff]
        g3_ref[0] = refs[1][0] + d13[:, ff:]
        g2_ref[0] = refs[2][0] + d2
    else:
        g1_ref[0] = d13[:, :ff]
        g3_ref[0] = d13[:, ff:]
        g2_ref[0] = d2


def row_kernel(slots, xa_ref, xb_ref, ca_ref, cb_ref, wo_ref, w2o_ref, wp_ref, w2p_ref, *r_refs):
    for q, (x_ref, c_ref) in enumerate(((xa_ref, ca_ref), (xb_ref, cb_ref))):
        x, c = x_ref[0], c_ref[0]
        y, dx = None, None
        for w_ref, v_ref in ((wo_ref, w2o_ref), (wp_ref, w2p_ref)):
            u, dab = act(nn(x, w_ref[0]), nt(c, v_ref[0]))
            py, pdx = nn(u, v_ref[0]), nt(dab, w_ref[0])
            y, dx = (py, pdx) if y is None else (y + py, dx + pdx)
        y, dx = y.astype(bf16), dx.astype(bf16)
        for b in range(2):
            if len(r_refs) == 8:
                r_refs[2 * q + b][0] = y[b * slots:(b + 1) * slots]
                r_refs[4 + 2 * q + b][0] = dx[b * slots:(b + 1) * slots]
            else:
                r_refs[2 * q + b][0, 0] = y[b * slots:(b + 1) * slots]
                r_refs[2 * q + b][0, 1] = dx[b * slots:(b + 1) * slots]


def names_of(groups, r_refs, part):
    names = []
    for gi, (lo, hi) in enumerate(groups):
        for q in range(4):
            ref = r_refs[4 * gi + q]
            for el in range(hi - lo):
                if len(ref.shape) == 4:
                    names.append((q, lo + el, lambda at, ref=ref, el=el: ref[el, part, pl.ds(at, 16), :]))
                else:
                    names.append((q, lo + el, lambda at, ref=ref, el=el: ref[el, pl.ds(at, 16), :]))
    return names


def fetch(names, w, slots, n_local, info_ref, win_ref, dst_ref):
    step = pl.program_id(0)
    for i, (q, el, read) in enumerate(names):
        first = win_ref[step, info_ref[q] * n_local + el]
        for piece in range(0, WIN, 16):
            at = pl.multiple_of(jnp.minimum(first + w * WIN + piece, slots - 16), 16)
            dst_ref[i * WIN + piece:i * WIN + piece + 16, :] = read(at)


def column(groups, n_local):
    width = 4 * sum(hi - lo for lo, hi in groups) * WIN
    lane = iota((1, width), 1)
    out, done = jnp.zeros((1, width), jnp.int32), 0
    for lo, hi in groups:
        for q in range(4):
            size = (hi - lo) * WIN
            out = jnp.where((lane >= done) & (lane < done + size), lane - done + (q * n_local + lo) * WIN, out)
            done += size
    return out.astype(f32)


def masks(code, w, col):
    if isinstance(w, int):
        return [jnp.where(col == code[:, 2 + k:3 + k], 1.0, 0.0) for k in range(2)]
    low = (w * WIN).astype(f32)
    out = []
    for k in range(2):
        rel = code[:, 9 + k:10 + k]
        at = jnp.where((rel >= low) & (rel < low + WIN), code[:, 7 + k:8 + k] + rel - low, -1.0)
        out.append(jnp.where(col == at, 1.0, 0.0))
    return out


def collect_y(code, w, col, rows_ref):
    return nn(jnp.concatenate(masks(code, w, col), axis=0).astype(bf16), rows_ref[...])


def collect_dx(code, w, col, rows_ref):
    m0, m1 = masks(code, w, col)
    return nn((m0 + m1).astype(bf16), rows_ref[...])


def further(win_ref, body):
    n_win = win_ref[pl.program_id(0), win_ref.shape[1] - 1]

    @pl.when(n_win > 1)
    def _():
        def run(w, carry):
            body(w)
            return carry

        lax.fori_loop(1, n_win, run, 0)


def combine_kernel(groups, slots, n_local, info_ref, win_ref, code_ref, *refs):
    n_r = 4 * len(groups)
    y0_ref, y1_ref, dx_ref, rows_ref = refs[n_r:]
    code = code_ref[...]
    rows = code.shape[0]
    col = column(groups, n_local)

    def collect(w):
        fetch(names_of(groups, refs[:n_r], 0), w, slots, n_local, info_ref, win_ref, rows_ref.at[0])
        fetch(names_of(groups, refs[:n_r], 1), w, slots, n_local, info_ref, win_ref, rows_ref.at[1])
        return collect_y(code, w, col, rows_ref.at[0]), collect_dx(code, w, col, rows_ref.at[1])

    y, dx = collect(0)
    y0_ref[...] = y[:rows].astype(bf16)
    y1_ref[...] = y[rows:].astype(bf16)
    dx_ref[...] = dx

    def more(w):
        y, dx = collect(w)
        y0_ref[...] = (y0_ref[...].astype(f32) + y[:rows]).astype(bf16)
        y1_ref[...] = (y1_ref[...].astype(f32) + y[rows:]).astype(bf16)
        dx_ref[...] = dx_ref[...] + dx

    further(win_ref, more)


def final_y_kernel(groups, slots, n_local, info_ref, win_ref, code_ref, *refs):
    n_r = 4 * len(groups)
    y0_ref, y1_ref, h_ref, d_ref, p_ref, coef_ref, stat_ref, out_ref, dz_ref, dr_ref, rows_ref, y_ref = refs[n_r:]
    code, p = code_ref[...], p_ref[...]
    n_experts = p.shape[1]
    rows = code.shape[0]
    col = column(groups, n_local)

    def collect(w):
        fetch(names_of(groups, refs[:n_r], 0), w, slots, n_local, info_ref, win_ref, rows_ref)
        return collect_y(code, w, col, rows_ref)

    y_ref[...] = collect(0)

    def more(w):
        y_ref[...] = y_ref[...] + collect(w)

    further(win_ref, more)
    y0 = y0_ref[...].astype(f32) + y_ref[:rows, :]
    y1 = y1_ref[...].astype(f32) + y_ref[rows:, :]
    e0, e1 = code[:, 0:1].astype(jnp.int32), code[:, 1:2].astype(jnp.int32)
    g0, g1, s = code[:, 4:5], code[:, 5:6], code[:, 6:7]
    h = h_ref[...]
    m = OUT_SCALE * d_ref[...].astype(f32)
    out_ref[...] = (h.astype(f32) + OUT_SCALE * (g0 * y0 + g1 * y1)).astype(bf16)
    dg0 = jnp.sum(m * y0, axis=1, keepdims=True)
    dg1 = jnp.sum(m * y1, axis=1, keepdims=True)
    mean = g0 * dg0 + g1 * dg1
    lane = iota(p.shape, 1)
    dp = (jnp.where(lane == e0, (dg0 - mean) / s, 0.0) + jnp.where(lane == e1, (dg1 - mean) / s, 0.0)
          + coef_ref[...])
    dz = p * (dp - jnp.sum(p * dp, axis=1, keepdims=True))
    dz_ref[...] = dz
    z3 = split3(dz)
    part = tn(z3[0], h) + (tn(z3[1], h) + tn(z3[2], h))

    @pl.when(pl.program_id(0) == 0)
    def _():
        dr_ref[...] = jnp.zeros_like(dr_ref)
        dr_ref[n_experts:n_experts + 1, 0:128] = stat_ref[1:2, :]

    dr_ref[0:n_experts, :] = dr_ref[0:n_experts, :] + part


def final_x_kernel(groups, slots, n_local, info_ref, win_ref, code_ref, *refs):
    n_r = 4 * len(groups)
    dx_ref, d_ref, dz_ref, wr_ref, dh_ref, rows_ref, x_ref, wt_ref = refs[n_r:]
    code = code_ref[...]
    col = column(groups, n_local)

    @pl.when(pl.program_id(0) == 0)
    def _():
        wt_ref[...] = wr_ref[...].T

    def collect(w):
        fetch(names_of(groups, refs[:n_r], 1), w, slots, n_local, info_ref, win_ref, rows_ref)
        return collect_dx(code, w, col, rows_ref)

    x_ref[...] = dx_ref[...] + collect(0)

    def more(w):
        x_ref[...] = x_ref[...] + collect(w)

    further(win_ref, more)
    z_hi, z_lo, _ = split3(dz_ref[...])
    w_hi, w_lo, _ = split3(wt_ref[...])
    back = nn(z_hi, w_hi) + (nn(z_lo, w_hi) + nn(z_hi, w_lo))
    dh_ref[...] = (d_ref[...].astype(f32) + x_ref[...] + back).astype(bf16)


def solution(mesh):
    ep_size = mesh.shape["ep"]
    etp_size = mesh.shape["etp"]
    n_dev = ep_size * etp_size
    all_axes = ("ep", "etp")
    tok_spec = P(all_axes, None)
    gate_spec = P("ep", None, "etp")
    down_spec = P("ep", "etp", None)

    def permute(v, dep, detp):
        pairs = [(t * ep_size + o, (t ^ detp) * ep_size + (o ^ dep)) for t in range(etp_size) for o in range(ep_size)]
        return lax.ppermute(v, ("etp", "ep"), pairs)

    def kernel(body, **kw):
        return pl.pallas_call(body, **kw)

    def layer(hidden, w_router, expert_ids, d_out, w_gate, w_up, w_down):
        tok_rows, d_model = hidden.shape
        n_experts = w_router.shape[1]
        n_local, _, ff = w_gate.shape
        n_tokens = tok_rows * n_dev
        capacity = (5 * n_tokens + 2 * n_experts - 1) // (2 * n_experts)
        slots = 7 * tok_rows // (2 * n_experts)
        ep, etp = lax.axis_index("ep"), lax.axis_index("etp")
        steps = tok_rows // TILE
        ep_info = jnp.stack([ep ^ q for q in range(4)]).astype(jnp.int32)
        sds = jax.ShapeDtypeStruct
        smem = pl.BlockSpec(memory_space=pltpu.SMEM)

        def whole(shape):
            return pl.BlockSpec(shape, lambda i: (0,) * len(shape))

        def tokens(width, tile=TILE):
            return pl.BlockSpec((tile, width), lambda i: (i, 0))

        def expert_block(shape, lo=0):
            return pl.BlockSpec((1,) + shape, lambda i: (i + lo,) + (0,) * len(shape))

        tile_ids = expert_ids.reshape(steps, TILE, 2).transpose(0, 2, 1).reshape(2 * steps, TILE)
        near_ids = [tile_ids] + [permute(tile_ids, r // etp_size, r % etp_size) for r in range(1, n_dev)]
        near_ids = jnp.stack(near_ids)
        rank = ep * etp_size + etp
        rank_info = jnp.concatenate([jnp.arange(n_dev, dtype=jnp.int32) ^ rank, (ep * n_local)[None]]).astype(jnp.int32)
        w13 = jnp.concatenate([w_gate, w_up], axis=2)

        hx, hy = permute(hidden, 2, 0), permute(hidden, 0, 1)
        dx_, dy_ = permute(d_out, 2, 0), permute(d_out, 0, 1)
        hd, dd = permute(hy, 2, 0), permute(dy_, 2, 0)
        core = lambda v: permute(v, 1, 0)
        h_pairs = {(0, 0): (hidden, core(hidden)), (1, 0): (hx, core(hx)), (0, 1): (hy, core(hy)), (1, 1): (hd, core(hd))}
        d_pairs = {(0, 0): (d_out, core(d_out)), (1, 0): (dx_, core(dx_)), (0, 1): (dy_, core(dy_)), (1, 1): (dd, core(dd))}
        partner = [(permute(w13[lo:hi], 0, 1), permute(w_down[lo:hi], 0, 1)) for lo, hi in CHUNKS]

        per_block = lambda *shape: pl.BlockSpec((1,) + shape, lambda i: (i,) + (0,) * len(shape))
        slot_rows, others, starts, wr3 = kernel(
            functools.partial(slot_kernel, capacity, slots, n_local),
            grid=(n_dev,),
            in_specs=[smem, whole(near_ids.shape), whole((d_model, n_experts))],
            out_specs=[per_block(steps * n_local, TILE), per_block(n_local, TILE), per_block(n_local, 128), whole((d_model, 128))],
            out_shape=[sds((n_dev, steps * n_local, TILE), f32), sds((n_dev, n_local, TILE), f32),
                       sds((n_dev, n_local, 128), jnp.int32), sds((d_model, 128), bf16)],
            scratch_shapes=[pltpu.VMEM((n_local, 128), f32)],
            compiler_params=params(), cost_estimate=cost(5e9),
        )(rank_info, near_ids, w_router)

        probs, code, wins, stats = kernel(
            functools.partial(route_kernel, n_experts, n_local),
            grid=(steps,),
            in_specs=[smem, tokens(d_model), whole((d_model, n_experts)), tokens(2)],
            out_specs=[tokens(n_experts), tokens(128), whole((8, 128)), whole((8, 128))],
            out_shape=[sds((tok_rows, n_experts), f32), sds((tok_rows, 128), f32), sds((8, 128), jnp.int32), sds((8, 128), f32)],
            compiler_params=params(), cost_estimate=cost(3e9),
        )(ep_info, hidden, w_router, expert_ids)

        def gather(pair):
            x, t = pair
            info = jnp.stack([(ep ^ (2 * x)) * etp_size + (etp ^ t), (ep ^ (2 * x + 1)) * etp_size + (etp ^ t), ep * n_local]).astype(jnp.int32)
            block = sds((n_local, 2 * slots, d_model), bf16)
            tile = pl.BlockSpec((TILE, d_model), lambda i: (jnp.minimum(i, steps - 1), 0))
            out = pl.BlockSpec((1, 2 * slots, d_model), lambda i: (jnp.maximum(i - steps, 0), 0, 0))
            return kernel(
                functools.partial(gather_kernel, slots, n_local, n_experts),
                grid=(steps + n_local,),
                in_specs=[smem, smem, whole(slot_rows.shape), whole(others.shape), whole(wr3.shape)] + [tile] * 4,
                out_specs=[out] * 2,
                out_shape=[block, block],
                scratch_shapes=[pltpu.VMEM((n_local * WIN, TILE), bf16)] + [pltpu.VMEM((2, n_local, slots + 64, d_model), bf16)] * 2,
                compiler_params=params(), cost_estimate=cost(8e9),
            )(info, starts, slot_rows, others, wr3, *h_pairs[pair], *d_pairs[pair])

        rows = {pair: gather(pair) for pair in h_pairs}
        row_block = expert_block((2 * slots, d_model))
        g13, g2 = expert_block((d_model, ff)), expert_block((ff, d_model))

        def grads(first, second, acc):
            (xa, ca), (xb, cb) = rows[first], rows[second]
            return kernel(
                functools.partial(grad_kernel, bool(acc)),
                grid=(n_local,),
                in_specs=[row_block] * 4 + [expert_block((d_model, 2 * ff)), expert_block((ff, d_model))] + [g13, g13, g2][:len(acc)],
                out_specs=[g13, g13, g2],
                out_shape=[sds((n_local, d_model, ff), f32)] * 2 + [sds((n_local, ff, d_model), f32)],
                input_output_aliases={6 + k: k for k in range(len(acc))},
                compiler_params=params(), cost_estimate=cost(25e9),
            )(xa, xb, ca, cb, w13, w_down, *acc)

        grad = grads((0, 0), (1, 0), ())
        g_gate, g_up, g_down = grads((0, 1), (1, 1), tuple(grad))

        def back(index):
            lo, hi = CHUNKS[index]
            (xa, ca), (xb, cb) = rows[(0, 0)], rows[(1, 0)]
            at = lambda shape: expert_block(shape, lo)
            outs = kernel(
                functools.partial(row_kernel, slots),
                grid=(hi - lo,),
                in_specs=[at((2 * slots, d_model))] * 4 + [at((d_model, 2 * ff)), at((ff, d_model)),
                          expert_block((d_model, 2 * ff)), expert_block((ff, d_model))],
                out_specs=[expert_block((slots, d_model))] * 8 if index == last else [expert_block((2, slots, d_model))] * 4,
                out_shape=[sds((hi - lo, slots, d_model), bf16)] * 8 if index == last else [sds((hi - lo, 2, slots, d_model), bf16)] * 4,
                compiler_params=params(), cost_estimate=cost(6e9 * (hi - lo)),
            )(xa, xb, ca, cb, w13, w_down, *partner[index])
            return [outs[i] if i % 4 == 0 else permute(outs[i], i % 4, 0) for i in range(len(outs))]

        last = len(CHUNKS) - 1
        returned = [back(i) for i in range(len(CHUNKS))]
        total = jnp.sum((near_ids.reshape(-1)[:, None] == jnp.arange(n_experts)[None, :]).astype(f32), axis=0)[None, :]
        coef = (AUX_COEF * n_experts / n_tokens / (2 * n_tokens)) * total

        def token_kernel(body, chunk_ids, arrays, extra, extra_specs, out_specs, out_shape, scratch):
            groups = tuple(CHUNKS[i] for i in chunk_ids)
            return kernel(
                functools.partial(body, groups, slots, n_local),
                grid=(steps,),
                in_specs=[smem, smem, tokens(128)] + [whole(r.shape) for r in arrays] + extra_specs,
                out_specs=out_specs, out_shape=out_shape, scratch_shapes=scratch,
                compiler_params=params(), cost_estimate=cost(8e9),
            )(ep_info, wins, code, *arrays, *extra)

        wide = tokens(d_model)
        width = lambda ids: 4 * sum(CHUNKS[i][1] - CHUNKS[i][0] for i in ids) * WIN
        early, late = (0, 1), (2, 3, last)
        y0, y1, dxs = token_kernel(
            combine_kernel, early, [r for i in early for r in returned[i]], (), [],
            [wide] * 3, [sds((tok_rows, d_model), bf16)] * 2 + [sds((tok_rows, d_model), f32)],
            [pltpu.VMEM((2, width(early), d_model), bf16)])
        ready = [r for i in late[:-1] for r in returned[i]]
        output, dz, d_rt = token_kernel(
            final_y_kernel, late, ready + returned[last][:4], (y0, y1, hidden, d_out, probs, coef, stats),
            [wide] * 4 + [tokens(n_experts), whole((1, n_experts)), whole((8, 128))],
            [wide, tokens(n_experts), whole((n_experts + 8, d_model))],
            [sds((tok_rows, d_model), bf16), sds((tok_rows, n_experts), f32), sds((n_experts + 8, d_model), f32)],
            [pltpu.VMEM((width(late), d_model), bf16), pltpu.VMEM((2 * TILE, d_model), f32)])
        (d_hidden,) = token_kernel(
            final_x_kernel, late, ready + returned[last][4:], (dxs, d_out, dz, w_router),
            [wide] * 2 + [tokens(n_experts), whole((d_model, n_experts))],
            [wide], [sds((tok_rows, d_model), bf16)],
            [pltpu.VMEM((width(late), d_model), bf16), pltpu.VMEM((TILE, d_model), f32), pltpu.VMEM((n_experts, d_model), f32)])
        for dep, detp in ((1, 0), (2, 0), (0, 1)):
            d_rt = d_rt + permute(d_rt, dep, detp)
        d_router = d_rt[:n_experts].T
        route_frac = total[0] / (2 * n_tokens)
        aux_loss = AUX_COEF * n_experts * jnp.sum(route_frac * (d_rt[n_experts, :n_experts] / n_tokens))
        return output, d_hidden, d_router, aux_loss, g_gate, g_up, g_down


    return jax.shard_map(layer, mesh=mesh, in_specs=(tok_spec, P(), tok_spec, tok_spec, gate_spec, gate_spec, down_spec), out_specs=(tok_spec, tok_spec, P(), P(), gate_spec, gate_spec, down_spec), check_vma=False)
```

```python
import functools
import jax
import jax.numpy as jnp
from jax import lax
from jax.experimental import pallas as pl
from jax.experimental.pallas import tpu as pltpu
from jax.sharding import PartitionSpec as P

AUX_COEF = 0.01
OUT_SCALE = 2.0
CHUNKS = ((0, 2), (2, 4), (4, 6), (6, 7), (7, 8))

f32, bf16 = jnp.float32, jnp.bfloat16
TILE = 256
WIN = 48


def nn(a, b):
    return jnp.dot(a, b, preferred_element_type=f32)


def nt(a, b):
    return lax.dot_general(a, b, (((1,), (1,)), ((), ())), preferred_element_type=f32)


def tn(a, b):
    return lax.dot_general(a, b, (((0,), (0,)), ((), ())), preferred_element_type=f32)


def split3(v):
    hi = v.astype(bf16)
    rest = v - hi.astype(f32)
    mid = rest.astype(bf16)
    return hi, mid, (rest - mid.astype(f32)).astype(bf16)


def ind(mask):
    return jnp.where(mask, 1.0, 0.0).astype(f32)


def rsum(v):
    return jnp.sum(v, axis=1, keepdims=True)


def csum(v):
    return jnp.sum(v, axis=0, keepdims=True)


def cols(v, *at):
    return [v[:, k:k + 1] for k in at]


def iota(shape, dim):
    return lax.broadcasted_iota(jnp.int32, shape, dim)


def params(**kw):
    return pltpu.CompilerParams(vmem_limit_bytes=60 * 2**20, **kw)


def cost(flops):
    return pl.CostEstimate(flops=int(flops), bytes_accessed=1 << 20, transcendentals=0)


def route_kernel(n_experts, n_local, info_ref, h_ref, wr_ref, ids_ref, p_ref, code_ref, win_ref, stat_ref):
    step = pl.program_id(0)

    @pl.when(step == 0)
    def _():
        stat_ref[...] = jnp.zeros_like(stat_ref)
        win_ref[...] = jnp.zeros_like(win_ref)

    w_hi, w_mid, w_lo = split3(wr_ref[...])
    h = h_ref[...]
    z = (nn(h, w_lo) + nn(h, w_mid)) + nn(h, w_hi)
    z = jnp.exp(z - jnp.max(z, axis=1, keepdims=True))
    p = z / rsum(z)
    p_ref[...] = p
    ids = ids_ref[...]
    lane = iota((TILE, n_experts), 1)
    e0, e1 = ids[:, 0:1], ids[:, 1:2]
    m0, m1 = lane == e0, lane == e1
    hist = ind(m0 | m1)
    before = (iota((TILE, TILE), 1) < iota((TILE, TILE), 0)).astype(f32).astype(bf16)
    seen = stat_ref[0:1, 0:n_experts]
    after = seen + csum(hist)
    start = jnp.floor(seen * (1.0 / 16)) * 16
    n_win = jnp.max(jnp.floor((after - start + (WIN - 1)) * (1.0 / WIN) + 1e-3), axis=1, keepdims=True)
    rank = nn(before, hist.astype(bf16)) + seen
    pick = lambda m, v: rsum(jnp.where(m, v, 0.0))
    p0, p1 = pick(m0, p), pick(m1, p)
    s = p0 + p1
    wide = iota((TILE, 128), 1)
    code = jnp.zeros((TILE, 128), f32)
    rel = rank - start
    name = iota((1, n_experts), 1)
    base = ((((name // n_local) ^ info_ref[0]) * n_local + name % n_local) * WIN).astype(f32)
    at = jnp.where(rel < WIN, base + rel, -1.0)
    spread = jnp.zeros_like(rel) + base
    for k, v in enumerate((e0.astype(f32), e1.astype(f32), pick(m0, at), pick(m1, at), p0 / s, p1 / s, s,
                           pick(m0, spread), pick(m1, spread), pick(m0, rel), pick(m1, rel))):
        code = jnp.where(wide == k, v, code)
    code_ref[...] = code
    win_ref[pl.ds(step, 1), 0:n_experts] = start.astype(jnp.int32)
    win_ref[pl.ds(step, 1), 127:128] = n_win.astype(jnp.int32)
    stat_ref[0:1, 0:n_experts] = after
    stat_ref[1:2, 0:n_experts] = stat_ref[1:2, 0:n_experts] + csum(p)


def slot_kernel(capacity, slots, n_local, info_ref, ids_ref, wr_ref, slot_ref, other_ref, start_ref, wr3_ref, total_ref):
    @pl.when(pl.program_id(0) == 0)
    def _():
        total_ref[...] = jnp.zeros_like(total_ref)
        wr3_ref[...] = jnp.zeros_like(wr3_ref)
        width = wr_ref.shape[1]
        for k, piece in enumerate(split3(wr_ref[...])):
            wr3_ref[:, k * width:(k + 1) * width] = piece

    steps = ids_ref.shape[1] // 2
    near = info_ref[pl.program_id(0)]
    expert = iota((n_local, TILE), 0) + info_ref[info_ref.shape[0] - 1]
    before = (iota((TILE, TILE), 0) < iota((TILE, TILE), 1)).astype(f32).astype(bf16)
    row = iota((TILE, TILE), 0).astype(f32)
    lane = iota((n_local, 128), 1)
    carry = jnp.zeros((n_local, 1), f32)
    starts = jnp.zeros((n_local, 128), f32)
    other = jnp.zeros((n_local, TILE), f32)
    for i in range(steps):
        e0, e1 = ids_ref[near, 2 * i:2 * i + 1, :], ids_ref[near, 2 * i + 1:2 * i + 2, :]
        m0, m1 = expert == e0, expert == e1
        hit = ind(m0 | m1)
        rank = nn(hit.astype(bf16), before) + carry
        slot_ref[0, i * n_local:(i + 1) * n_local, :] = jnp.where(m0 | m1, rank, -1.0)
        starts = jnp.where(lane == i, carry, starts)
        for m, e in ((m0, e1), (m1, e0)):
            pos = csum(jnp.where(m, rank + 1.0, 0.0)) - 1.0
            one = ind(row == pos).astype(bf16)
            other = other + nt(jnp.where(m, e.astype(f32), 0.0).astype(bf16), one)
        carry = carry + rsum(hit)
    other_ref[0] = other
    prefix = total_ref[:, 0:1]
    room = jnp.clip(capacity - prefix, 0.0, float(slots))
    starts = jnp.where(lane == steps, carry, jnp.where(lane == steps + 1, jnp.minimum(room, carry), starts))
    start_ref[0] = starts.astype(jnp.int32)
    total_ref[...] = total_ref[...] + carry


def gather_kernel(slots, n_local, n_experts, info_ref, start_ref, slot_ref, other_ref, wr3_ref, ha_ref, hb_ref, da_ref, db_ref,
                  x_ref, c_ref, m_ref, xs_ref, ds_ref):
    step = pl.program_id(0)
    steps = pl.num_programs(0) - n_local

    @pl.when(step < steps)
    def _():
        row = iota((WIN, TILE), 0)
        for b, (h_ref, d_ref) in enumerate(((ha_ref, da_ref), (hb_ref, db_ref))):
            j = info_ref[b]
            first = [(start_ref[j, e, step] // 16) * 16 for e in range(n_local)]
            span = functools.reduce(jnp.maximum, [start_ref[j, e, step + 1] - first[e] for e in range(n_local)])

            def window(w, carry):
                for e in range(n_local):
                    slot = slot_ref[j, pl.ds(step * n_local + e, 1), :]
                    hit = (row + (first[e] + w * WIN)).astype(f32) == slot
                    m_ref[e * WIN:(e + 1) * WIN, :] = ind(hit).astype(bf16)
                m = m_ref[...]
                for src, dst in ((h_ref, xs_ref), (d_ref, ds_ref)):
                    r = nn(m, src[...]).astype(bf16)
                    for e in range(n_local):
                        at = pl.multiple_of(jnp.minimum(first[e] + w * WIN, slots + 16), 16)
                        old = dst[b, e, pl.ds(at, 16), :]
                        keep = iota((16, 1), 0) + at < start_ref[j, e, step]
                        head = r[e * WIN:e * WIN + 16].astype(f32)
                        dst[b, e, pl.ds(at, 16), :] = jnp.where(keep, old.astype(f32), head).astype(bf16)
                        dst[b, e, pl.ds(pl.multiple_of(at + 16, 16), WIN - 16), :] = r[e * WIN + 16:(e + 1) * WIN]
                return carry

            lax.fori_loop(0, (span + WIN - 1) // WIN, window, 0)

    @pl.when(step >= steps)
    def _():
        e = step - steps
        lane = iota((slots, 128), 1)
        for b in range(2):
            j = info_ref[b]
            kept = iota((slots, 1), 0) < start_ref[j, e, steps + 1]
            x = jnp.where(kept, xs_ref[b, e, 0:slots, :].astype(f32), 0.0)
            d = jnp.where(kept, ds_ref[b, e, 0:slots, :].astype(f32), 0.0)
            x = x.astype(bf16)
            x_ref[0, b * slots:(b + 1) * slots, :] = x
            z = nn(x, wr3_ref[...])
            other = other_ref[j].T[0:slots, :]
            other = rsum(jnp.where(iota((slots, n_local), 1) == e, other, 0.0))
            name = lane % n_experts
            here = rsum(jnp.where(name == info_ref[2] + e, z, 0.0))
            there = rsum(jnp.where(name == other.astype(jnp.int32), z, 0.0))
            g = 1.0 / (1.0 + jnp.exp(there - here))
            c_ref[0, b * slots:(b + 1) * slots, :] = (g * (OUT_SCALE * d)).astype(bf16)


def act(ab, du):
    ff = du.shape[1]
    a, b = ab[:, :ff], ab[:, ff:]
    sig = jax.nn.sigmoid(a)
    silu = a * sig
    u = (silu * b).astype(bf16)
    da = (du * b * sig * (1.0 + a * (1.0 - sig))).astype(bf16)
    db = (du * silu).astype(bf16)
    return u, jnp.concatenate([da, db], axis=1)


def grad_kernel(accumulate, xa_ref, xb_ref, ca_ref, cb_ref, w13_ref, w2_ref, *refs):
    g1_ref, g3_ref, g2_ref = refs[-3:]
    ff = w2_ref.shape[1]
    d13, d2 = None, None
    for x_ref, c_ref in ((xa_ref, ca_ref), (xb_ref, cb_ref)):
        x, c = x_ref[0], c_ref[0]
        u, dab = act(nn(x, w13_ref[0]), nt(c, w2_ref[0]))
        p13, p2 = tn(x, dab), tn(u, c)
        d13, d2 = (p13, p2) if d13 is None else (d13 + p13, d2 + p2)
    if accumulate:
        g1_ref[0] = refs[0][0] + d13[:, :ff]
        g3_ref[0] = refs[1][0] + d13[:, ff:]
        g2_ref[0] = refs[2][0] + d2
    else:
        g1_ref[0] = d13[:, :ff]
        g3_ref[0] = d13[:, ff:]
        g2_ref[0] = d2


def row_kernel(slots, xa_ref, xb_ref, ca_ref, cb_ref, wo_ref, w2o_ref, wp_ref, w2p_ref, *r_refs):
    for q, (x_ref, c_ref) in enumerate(((xa_ref, ca_ref), (xb_ref, cb_ref))):
        x, c = x_ref[0], c_ref[0]
        y, dx = None, None
        for w_ref, v_ref in ((wo_ref, w2o_ref), (wp_ref, w2p_ref)):
            u, dab = act(nn(x, w_ref[0]), nt(c, v_ref[0]))
            py, pdx = nn(u, v_ref[0]), nt(dab, w_ref[0])
            y, dx = (py, pdx) if y is None else (y + py, dx + pdx)
        y, dx = y.astype(bf16), dx.astype(bf16)
        for b in range(2):
            if len(r_refs) == 8:
                r_refs[2 * q + b][0] = y[b * slots:(b + 1) * slots]
                r_refs[4 + 2 * q + b][0] = dx[b * slots:(b + 1) * slots]
            else:
                r_refs[2 * q + b][0, 0] = y[b * slots:(b + 1) * slots]
                r_refs[2 * q + b][0, 1] = dx[b * slots:(b + 1) * slots]


def names_of(groups, r_refs, part):
    names = []
    for gi, (lo, hi) in enumerate(groups):
        for q in range(4):
            ref = r_refs[4 * gi + q]
            for el in range(hi - lo):
                if len(ref.shape) == 4:
                    names.append((q, lo + el, lambda at, ref=ref, el=el: ref[el, part, pl.ds(at, 16), :]))
                else:
                    names.append((q, lo + el, lambda at, ref=ref, el=el: ref[el, pl.ds(at, 16), :]))
    return names


def fetch(names, w, slots, n_local, info_ref, win_ref, dst_ref):
    step = pl.program_id(0)
    for i, (q, el, read) in enumerate(names):
        first = win_ref[step, info_ref[q] * n_local + el]
        for piece in range(0, WIN, 16):
            at = pl.multiple_of(jnp.minimum(first + w * WIN + piece, slots - 16), 16)
            dst_ref[i * WIN + piece:i * WIN + piece + 16, :] = read(at)


def column(groups, n_local):
    width = 4 * sum(hi - lo for lo, hi in groups) * WIN
    lane = iota((1, width), 1)
    out, done = jnp.zeros((1, width), jnp.int32), 0
    for lo, hi in groups:
        for q in range(4):
            size = (hi - lo) * WIN
            out = jnp.where((lane >= done) & (lane < done + size), lane - done + (q * n_local + lo) * WIN, out)
            done += size
    return out.astype(f32)


def masks(code, w, col):
    if isinstance(w, int):
        return [jnp.where(col == code[:, 2 + k:3 + k], 1.0, 0.0) for k in range(2)]
    low = (w * WIN).astype(f32)
    out = []
    for k in range(2):
        rel = code[:, 9 + k:10 + k]
        at = jnp.where((rel >= low) & (rel < low + WIN), code[:, 7 + k:8 + k] + rel - low, -1.0)
        out.append(ind(col == at))
    return out


def collect_y(code, w, col, rows_ref):
    return nn(jnp.concatenate(masks(code, w, col), axis=0).astype(bf16), rows_ref[...])


def collect_dx(code, w, col, rows_ref):
    m0, m1 = masks(code, w, col)
    return nn((m0 + m1).astype(bf16), rows_ref[...])


def further(win_ref, body):
    n_win = win_ref[pl.program_id(0), win_ref.shape[1] - 1]

    @pl.when(n_win > 1)
    def _():
        def run(w, carry):
            body(w)
            return carry

        lax.fori_loop(1, n_win, run, 0)


def combine_kernel(groups, slots, n_local, info_ref, win_ref, code_ref, *refs):
    n_r = 4 * len(groups)
    y0_ref, y1_ref, dx_ref, rows_ref = refs[n_r:]
    code = code_ref[...]
    rows = code.shape[0]
    col = column(groups, n_local)

    def collect(w):
        fetch(names_of(groups, refs[:n_r], 0), w, slots, n_local, info_ref, win_ref, rows_ref.at[0])
        fetch(names_of(groups, refs[:n_r], 1), w, slots, n_local, info_ref, win_ref, rows_ref.at[1])
        return collect_y(code, w, col, rows_ref.at[0]), collect_dx(code, w, col, rows_ref.at[1])

    y, dx = collect(0)
    y0_ref[...] = y[:rows].astype(bf16)
    y1_ref[...] = y[rows:].astype(bf16)
    dx_ref[...] = dx

    def more(w):
        y, dx = collect(w)
        y0_ref[...] = (y0_ref[...].astype(f32) + y[:rows]).astype(bf16)
        y1_ref[...] = (y1_ref[...].astype(f32) + y[rows:]).astype(bf16)
        dx_ref[...] = dx_ref[...] + dx

    further(win_ref, more)


def final_y_kernel(groups, slots, n_local, info_ref, win_ref, code_ref, *refs):
    n_r = 4 * len(groups)
    y0_ref, y1_ref, h_ref, d_ref, p_ref, coef_ref, stat_ref, out_ref, dz_ref, dr_ref, rows_ref, y_ref = refs[n_r:]
    code, p = code_ref[...], p_ref[...]
    n_experts = p.shape[1]
    rows = code.shape[0]
    col = column(groups, n_local)

    def collect(w):
        fetch(names_of(groups, refs[:n_r], 0), w, slots, n_local, info_ref, win_ref, rows_ref)
        return collect_y(code, w, col, rows_ref)

    y_ref[...] = jnp.zeros_like(y_ref)

    def more(w):
        y_ref[...] = y_ref[...] + collect(w)

    further(win_ref, more)
    y = y_ref[...] + collect(0)
    y0 = y0_ref[...].astype(f32) + y[:rows]
    y1 = y1_ref[...].astype(f32) + y[rows:]
    e0, e1, g0, g1, s = cols(code, 0, 1, 4, 5, 6)
    h = h_ref[...]
    m = OUT_SCALE * d_ref[...].astype(f32)
    out_ref[...] = (h.astype(f32) + OUT_SCALE * (g0 * y0 + g1 * y1)).astype(bf16)
    dg0 = rsum(m * y0)
    dg1 = rsum(m * y1)
    mean = g0 * dg0 + g1 * dg1
    lane = iota(p.shape, 1).astype(f32)
    dp = (jnp.where(lane == e0, (dg0 - mean) / s, 0.0) + jnp.where(lane == e1, (dg1 - mean) / s, 0.0)
          + coef_ref[...])
    dz = p * (dp - rsum(p * dp))
    dz_ref[...] = dz
    z3 = split3(dz)
    part = tn(z3[0], h) + (tn(z3[1], h) + tn(z3[2], h))

    @pl.when(pl.program_id(0) == 0)
    def _():
        dr_ref[...] = jnp.zeros_like(dr_ref)
        dr_ref[n_experts:n_experts + 1, 0:128] = stat_ref[1:2, :]

    dr_ref[0:n_experts, :] = dr_ref[0:n_experts, :] + part


def final_x_kernel(groups, slots, n_local, info_ref, win_ref, code_ref, *refs):
    n_r = 4 * len(groups)
    dx_ref, d_ref, dz_ref, wr_ref, dh_ref, rows_ref, x_ref, wt_ref = refs[n_r:]
    code = code_ref[...]
    col = column(groups, n_local)

    @pl.when(pl.program_id(0) == 0)
    def _():
        wt_ref[...] = wr_ref[...].T

    def collect(w):
        fetch(names_of(groups, refs[:n_r], 1), w, slots, n_local, info_ref, win_ref, rows_ref)
        return collect_dx(code, w, col, rows_ref)

    x_ref[...] = dx_ref[...]

    def more(w):
        x_ref[...] = x_ref[...] + collect(w)

    further(win_ref, more)
    dx = x_ref[...] + collect(0)
    z_hi, z_lo, _ = split3(dz_ref[...])
    w_hi, w_lo, _ = split3(wt_ref[...])
    back = nn(z_hi, w_hi) + (nn(z_lo, w_hi) + nn(z_hi, w_lo))
    dh_ref[...] = (d_ref[...].astype(f32) + dx + back).astype(bf16)


def solution(mesh):
    ep_size = mesh.shape["ep"]
    etp_size = mesh.shape["etp"]
    n_dev = ep_size * etp_size
    all_axes = ("ep", "etp")
    tok_spec = P(all_axes, None)
    gate_spec = P("ep", None, "etp")
    down_spec = P("ep", "etp", None)

    def permute(v, dep, detp):
        pairs = [(t * ep_size + o, (t ^ detp) * ep_size + (o ^ dep)) for t in range(etp_size) for o in range(ep_size)]
        return lax.ppermute(v, ("etp", "ep"), pairs)

    def kernel(body, **kw):
        return pl.pallas_call(body, **kw)

    def layer(hidden, w_router, expert_ids, d_out, w_gate, w_up, w_down):
        tok_rows, d_model = hidden.shape
        n_experts = w_router.shape[1]
        n_local, _, ff = w_gate.shape
        n_tokens = tok_rows * n_dev
        capacity = (5 * n_tokens + 2 * n_experts - 1) // (2 * n_experts)
        slots = 7 * tok_rows // (2 * n_experts)
        ep, etp = lax.axis_index("ep"), lax.axis_index("etp")
        steps = tok_rows // TILE
        ep_info = jnp.stack([ep ^ q for q in range(4)]).astype(jnp.int32)
        sds = jax.ShapeDtypeStruct
        smem = pl.BlockSpec(memory_space=pltpu.SMEM)

        def whole(shape):
            return pl.BlockSpec(shape, lambda i: (0,) * len(shape))

        def tokens(width, tile=TILE):
            return pl.BlockSpec((tile, width), lambda i: (i, 0))

        def expert_block(shape, lo=0):
            return pl.BlockSpec((1,) + shape, lambda i: (i + lo,) + (0,) * len(shape))

        tile_ids = expert_ids.reshape(steps, TILE, 2).transpose(0, 2, 1).reshape(2 * steps, TILE)
        near_ids = [tile_ids] + [permute(tile_ids, r // etp_size, r % etp_size) for r in range(1, n_dev)]
        near_ids = jnp.stack(near_ids)
        rank = ep * etp_size + etp
        rank_info = jnp.concatenate([jnp.arange(n_dev, dtype=jnp.int32) ^ rank, (ep * n_local)[None]]).astype(jnp.int32)
        w13 = jnp.concatenate([w_gate, w_up], axis=2)

        hx, hy = permute(hidden, 2, 0), permute(hidden, 0, 1)
        dx_, dy_ = permute(d_out, 2, 0), permute(d_out, 0, 1)
        hd, dd = permute(hy, 2, 0), permute(dy_, 2, 0)
        core = lambda v: permute(v, 1, 0)
        h_pairs = {(0, 0): (hidden, core(hidden)), (1, 0): (hx, core(hx)), (0, 1): (hy, core(hy)), (1, 1): (hd, core(hd))}
        d_pairs = {(0, 0): (d_out, core(d_out)), (1, 0): (dx_, core(dx_)), (0, 1): (dy_, core(dy_)), (1, 1): (dd, core(dd))}
        partner = [(permute(w13[lo:hi], 0, 1), permute(w_down[lo:hi], 0, 1)) for lo, hi in CHUNKS]

        per_block = lambda *shape: pl.BlockSpec((1,) + shape, lambda i: (i,) + (0,) * len(shape))
        slot_rows, others, starts, wr3 = kernel(
            functools.partial(slot_kernel, capacity, slots, n_local),
            grid=(n_dev,),
            in_specs=[smem, whole(near_ids.shape), whole((d_model, n_experts))],
            out_specs=[per_block(steps * n_local, TILE), per_block(n_local, TILE), per_block(n_local, 128), whole((d_model, 128))],
            out_shape=[sds((n_dev, steps * n_local, TILE), f32), sds((n_dev, n_local, TILE), f32),
                       sds((n_dev, n_local, 128), jnp.int32), sds((d_model, 128), bf16)],
            scratch_shapes=[pltpu.VMEM((n_local, 128), f32)],
            compiler_params=params(), cost_estimate=cost(5e9),
        )(rank_info, near_ids, w_router)

        probs, code, wins, stats = kernel(
            functools.partial(route_kernel, n_experts, n_local),
            grid=(steps,),
            in_specs=[smem, tokens(d_model), whole((d_model, n_experts)), tokens(2)],
            out_specs=[tokens(n_experts), tokens(128), whole((8, 128)), whole((8, 128))],
            out_shape=[sds((tok_rows, n_experts), f32), sds((tok_rows, 128), f32), sds((8, 128), jnp.int32), sds((8, 128), f32)],
            compiler_params=params(), cost_estimate=cost(3e9),
        )(ep_info, hidden, w_router, expert_ids)

        def gather(pair):
            x, t = pair
            info = jnp.stack([(ep ^ (2 * x)) * etp_size + (etp ^ t), (ep ^ (2 * x + 1)) * etp_size + (etp ^ t), ep * n_local]).astype(jnp.int32)
            block = sds((n_local, 2 * slots, d_model), bf16)
            tile = pl.BlockSpec((TILE, d_model), lambda i: (jnp.minimum(i, steps - 1), 0))
            out = pl.BlockSpec((1, 2 * slots, d_model), lambda i: (jnp.maximum(i - steps, 0), 0, 0))
            return kernel(
                functools.partial(gather_kernel, slots, n_local, n_experts),
                grid=(steps + n_local,),
                in_specs=[smem, smem, whole(slot_rows.shape), whole(others.shape), whole(wr3.shape)] + [tile] * 4,
                out_specs=[out] * 2,
                out_shape=[block, block],
                scratch_shapes=[pltpu.VMEM((n_local * WIN, TILE), bf16)] + [pltpu.VMEM((2, n_local, slots + 64, d_model), bf16)] * 2,
                compiler_params=params(), cost_estimate=cost(8e9),
            )(info, starts, slot_rows, others, wr3, *h_pairs[pair], *d_pairs[pair])

        rows = {pair: gather(pair) for pair in h_pairs}

        def grads(first, second, acc, lo, hi):
            (xa, ca), (xb, cb) = rows[first], rows[second]
            at = lambda shape: expert_block(shape, lo)
            g13, g2 = at((d_model, ff)), at((ff, d_model))
            return kernel(
                functools.partial(grad_kernel, bool(acc)),
                grid=(hi - lo,),
                in_specs=[at((2 * slots, d_model))] * 4 + [at((d_model, 2 * ff)), at((ff, d_model))] + [g13, g13, g2][:len(acc)],
                out_specs=[g13, g13, g2],
                out_shape=[sds((n_local, d_model, ff), f32)] * 2 + [sds((n_local, ff, d_model), f32)],
                input_output_aliases={6 + k: k for k in range(len(acc))},
                compiler_params=params(), cost_estimate=cost(3e9 * (hi - lo)),
            )(xa, xb, ca, cb, w13, w_down, *acc)

        grad = grads((0, 0), (1, 0), (), 0, n_local)
        grad = grads((0, 1), (1, 1), tuple(grad), 0, n_local // 2)
        g_gate, g_up, g_down = grads((0, 1), (1, 1), tuple(grad), n_local // 2, n_local)

        def back(index):
            lo, hi = CHUNKS[index]
            (xa, ca), (xb, cb) = rows[(0, 0)], rows[(1, 0)]
            at = lambda shape: expert_block(shape, lo)
            outs = kernel(
                functools.partial(row_kernel, slots),
                grid=(hi - lo,),
                in_specs=[at((2 * slots, d_model))] * 4 + [at((d_model, 2 * ff)), at((ff, d_model)),
                          expert_block((d_model, 2 * ff)), expert_block((ff, d_model))],
                out_specs=[expert_block((slots, d_model))] * 8 if index >= split else [expert_block((2, slots, d_model))] * 4,
                out_shape=[sds((hi - lo, slots, d_model), bf16)] * 8 if index >= split else [sds((hi - lo, 2, slots, d_model), bf16)] * 4,
                compiler_params=params(), cost_estimate=cost(6e9 * (hi - lo)),
            )(xa, xb, ca, cb, w13, w_down, *partner[index])
            return [outs[i] if i % 4 == 0 else permute(outs[i], i % 4, 0) for i in range(len(outs))]

        last = len(CHUNKS) - 1
        split = last - 1
        returned = [back(i) for i in range(len(CHUNKS))]
        total = jnp.sum((near_ids.reshape(-1)[:, None] == jnp.arange(n_experts)[None, :]).astype(f32), axis=0)[None, :]
        coef = (AUX_COEF * n_experts / n_tokens / (2 * n_tokens)) * total

        def token_kernel(body, chunk_ids, arrays, extra, extra_specs, out_specs, out_shape, scratch):
            groups = tuple(CHUNKS[i] for i in chunk_ids)
            return kernel(
                functools.partial(body, groups, slots, n_local),
                grid=(steps,),
                in_specs=[smem, smem, tokens(128)] + [whole(r.shape) for r in arrays] + extra_specs,
                out_specs=out_specs, out_shape=out_shape, scratch_shapes=scratch,
                compiler_params=params(), cost_estimate=cost(8e9),
            )(ep_info, wins, code, *arrays, *extra)

        wide = tokens(d_model)
        width = lambda ids: 4 * sum(CHUNKS[i][1] - CHUNKS[i][0] for i in ids) * WIN
        early, late = (0, 1), (2, 3, last)
        y0, y1, dxs = token_kernel(
            combine_kernel, early, [r for i in early for r in returned[i]], (), [],
            [wide] * 3, [sds((tok_rows, d_model), bf16)] * 2 + [sds((tok_rows, d_model), f32)],
            [pltpu.VMEM((2, width(early), d_model), bf16)])
        half = lambda k: [r for i in late for r in (returned[i] if len(returned[i]) == 4 else returned[i][4 * k:4 * k + 4])]
        output, dz, d_rt = token_kernel(
            final_y_kernel, late, half(0), (y0, y1, hidden, d_out, probs, coef, stats),
            [wide] * 4 + [tokens(n_experts), whole((1, n_experts)), whole((8, 128))],
            [wide, tokens(n_experts), whole((n_experts + 8, d_model))],
            [sds((tok_rows, d_model), bf16), sds((tok_rows, n_experts), f32), sds((n_experts + 8, d_model), f32)],
            [pltpu.VMEM((width(late), d_model), bf16), pltpu.VMEM((2 * TILE, d_model), f32)])
        (d_hidden,) = token_kernel(
            final_x_kernel, late, half(1), (dxs, d_out, dz, w_router),
            [wide] * 2 + [tokens(n_experts), whole((d_model, n_experts))],
            [wide], [sds((tok_rows, d_model), bf16)],
            [pltpu.VMEM((width(late), d_model), bf16), pltpu.VMEM((TILE, d_model), f32), pltpu.VMEM((n_experts, d_model), f32)])
        for dep, detp in ((1, 0), (2, 0), (0, 1)):
            d_rt = d_rt + permute(d_rt, dep, detp)
        d_router = d_rt[:n_experts].T
        route_frac = total[0] / (2 * n_tokens)
        aux_loss = AUX_COEF * n_experts * jnp.sum(route_frac * (d_rt[n_experts, :n_experts] / n_tokens))
        return output, d_hidden, d_router, aux_loss, g_gate, g_up, g_down


    return jax.shard_map(layer, mesh=mesh, in_specs=(tok_spec, P(), tok_spec, tok_spec, gate_spec, gate_spec, down_spec), out_specs=(tok_spec, tok_spec, P(), P(), gate_spec, gate_spec, down_spec), check_vma=False)
```

```python
import functools
import jax
import jax.numpy as jnp
from jax import lax
from jax.experimental import pallas as pl
from jax.experimental.pallas import tpu as pltpu
from jax.sharding import PartitionSpec as P

AUX_COEF = 0.01
OUT_SCALE = 2.0
SIZES = (2, 2, 1, 1, 1, 1)
CHUNKS = tuple((sum(SIZES[:i]), sum(SIZES[:i]) + n) for i, n in enumerate(SIZES))

f32, bf16 = jnp.float32, jnp.bfloat16
TILE = 256
GROUP = 2
WIN = 48


def nn(a, b):
    return jnp.dot(a, b, preferred_element_type=f32)


def nt(a, b):
    return lax.dot_general(a, b, (((1,), (1,)), ((), ())), preferred_element_type=f32)


def tn(a, b):
    return lax.dot_general(a, b, (((0,), (0,)), ((), ())), preferred_element_type=f32)


def split3(v):
    hi = v.astype(bf16)
    rest = v - hi.astype(f32)
    mid = rest.astype(bf16)
    return hi, mid, (rest - mid.astype(f32)).astype(bf16)


def ind(mask):
    return jnp.where(mask, 1.0, 0.0).astype(f32)


def keep(mask, v):
    return jnp.where(mask, v, 0.0)


def rsum(v):
    return jnp.sum(v, axis=1, keepdims=True)


def csum(v):
    return jnp.sum(v, axis=0, keepdims=True)


def cols(v, *at):
    return [v[:, k:k + 1] for k in at]


def iota(shape, dim):
    return lax.broadcasted_iota(jnp.int32, shape, dim)


def params(**kw):
    return pltpu.CompilerParams(vmem_limit_bytes=60 * 2**20, **kw)


def cost(flops):
    return pl.CostEstimate(flops=int(flops), bytes_accessed=1 << 20, transcendentals=0)


def route_kernel(n_experts, n_local, info_ref, h_ref, wr_ref, ids_ref, p_ref, code_ref, win_ref, stat_ref):
    step = pl.program_id(0)

    @pl.when(step == 0)
    def _():
        stat_ref[...] = jnp.zeros_like(stat_ref)
        win_ref[...] = jnp.zeros_like(win_ref)

    w_hi, w_mid, w_lo = split3(wr_ref[...])
    h = h_ref[...]
    z = (nn(h, w_lo) + nn(h, w_mid)) + nn(h, w_hi)
    z = jnp.exp(z - jnp.max(z, axis=1, keepdims=True))
    p = z / rsum(z)
    p_ref[...] = p
    ids = ids_ref[...]
    lane = iota((TILE, n_experts), 1)
    e0, e1 = cols(ids, 0, 1)
    m0, m1 = lane == e0, lane == e1
    hist = ind(m0 | m1)
    before = (iota((TILE, TILE), 1) < iota((TILE, TILE), 0)).astype(f32).astype(bf16)
    seen = stat_ref[0:1, 0:n_experts]
    after = seen + csum(hist)
    start = jnp.floor(seen * (1.0 / 16)) * 16
    n_win = jnp.max(jnp.floor((after - start + (WIN - 1)) * (1.0 / WIN) + 1e-3), axis=1, keepdims=True)
    rank = nn(before, hist.astype(bf16)) + seen
    pick = lambda m, v: rsum(keep(m, v))
    p0, p1 = pick(m0, p), pick(m1, p)
    s = p0 + p1
    wide = iota((TILE, 128), 1)
    code = jnp.zeros((TILE, 128), f32)
    rel = rank - start
    name = iota((1, n_experts), 1)
    base = ((((name // n_local) ^ info_ref[0]) * n_local + name % n_local) * WIN).astype(f32)
    at = jnp.where(rel < WIN, base + rel, -1.0)
    spread = jnp.zeros_like(rel) + base
    for k, v in enumerate((e0.astype(f32), e1.astype(f32), pick(m0, at), pick(m1, at), p0 / s, p1 / s, s,
                           pick(m0, spread), pick(m1, spread), pick(m0, rel), pick(m1, rel))):
        code = jnp.where(wide == k, v, code)
    code_ref[...] = code
    win_ref[pl.ds(step, 1), 0:n_experts] = start.astype(jnp.int32)
    win_ref[pl.ds(step, 1), 127:128] = n_win.astype(jnp.int32)
    stat_ref[0:1, 0:n_experts] = after
    stat_ref[1:2, 0:n_experts] = stat_ref[1:2, 0:n_experts] + csum(p)


def slot_kernel(capacity, slots, n_local, info_ref, ids_ref, wr_ref, slot_ref, other_ref, start_ref, wr3_ref, total_ref):
    @pl.when(pl.program_id(0) == 0)
    def _():
        total_ref[...] = jnp.zeros_like(total_ref)
        wr3_ref[...] = jnp.zeros_like(wr3_ref)
        width = wr_ref.shape[1]
        for k, piece in enumerate(split3(wr_ref[...])):
            wr3_ref[:, k * width:(k + 1) * width] = piece

    steps = ids_ref.shape[1] // 2
    near = info_ref[pl.program_id(0)]
    expert = iota((n_local, TILE), 0) + info_ref[info_ref.shape[0] - 1]
    before = (iota((TILE, TILE), 0) < iota((TILE, TILE), 1)).astype(f32).astype(bf16)
    row = iota((TILE, TILE), 0).astype(f32)
    lane = iota((n_local, 128), 1)
    carry = jnp.zeros((n_local, 1), f32)
    starts = jnp.zeros((n_local, 128), f32)
    other = jnp.zeros((n_local, TILE), f32)
    for i in range(steps):
        e0, e1 = ids_ref[near, 2 * i:2 * i + 1, :], ids_ref[near, 2 * i + 1:2 * i + 2, :]
        m0, m1 = expert == e0, expert == e1
        hit = ind(m0 | m1)
        rank = nn(hit.astype(bf16), before) + carry
        slot_ref[0, i * n_local:(i + 1) * n_local, :] = jnp.where(m0 | m1, rank, -1.0)
        starts = jnp.where(lane == i, carry, starts)
        for m, e in ((m0, e1), (m1, e0)):
            pos = csum(keep(m, rank + 1.0)) - 1.0
            one = ind(row == pos).astype(bf16)
            other = other + nt(keep(m, e.astype(f32)).astype(bf16), one)
        carry = carry + rsum(hit)
    other_ref[0] = other
    prefix = total_ref[:, 0:1]
    room = jnp.clip(capacity - prefix, 0.0, float(slots))
    starts = jnp.where(lane == steps, carry, jnp.where(lane == steps + 1, jnp.minimum(room, carry), starts))
    start_ref[0] = starts.astype(jnp.int32)
    total_ref[...] = total_ref[...] + carry


def gather_kernel(slots, n_local, n_experts, info_ref, start_ref, slot_ref, other_ref, wr3_ref, ha_ref, hb_ref, da_ref, db_ref,
                  x_ref, c_ref, m_ref, xs_ref, ds_ref):
    step = pl.program_id(0)
    group = x_ref.shape[0]
    steps = pl.num_programs(0) - n_local // group

    @pl.when(step < steps)
    def _():
        row = iota((WIN, TILE), 0)

        def one_tile(sub, carry):
            tile = step * group + sub
            part = pl.ds(pl.multiple_of(sub * TILE, TILE), TILE)
            for b, (h_ref, d_ref) in enumerate(((ha_ref, da_ref), (hb_ref, db_ref))):
                j = info_ref[b]
                first = [(start_ref[j, e, tile] // 16) * 16 for e in range(n_local)]
                span = functools.reduce(jnp.maximum, [start_ref[j, e, tile + 1] - first[e] for e in range(n_local)])

                def window(w, carry):
                    for e in range(n_local):
                        slot = slot_ref[j, pl.ds(tile * n_local + e, 1), :]
                        hit = (row + (first[e] + w * WIN)).astype(f32) == slot
                        m_ref[e * WIN:(e + 1) * WIN, :] = ind(hit).astype(bf16)
                    m = m_ref[...]
                    for src, dst in ((h_ref, xs_ref), (d_ref, ds_ref)):
                        r = nn(m, src[part, :]).astype(bf16)
                        for e in range(n_local):
                            at = pl.multiple_of(jnp.minimum(first[e] + w * WIN, slots + 16), 16)
                            old = dst[b, e, pl.ds(at, 16), :]
                            older = iota((16, 1), 0) + at < start_ref[j, e, tile]
                            head = r[e * WIN:e * WIN + 16].astype(f32)
                            dst[b, e, pl.ds(at, 16), :] = jnp.where(older, old.astype(f32), head).astype(bf16)
                            dst[b, e, pl.ds(pl.multiple_of(at + 16, 16), WIN - 16), :] = r[e * WIN + 16:(e + 1) * WIN]
                    return carry

                lax.fori_loop(0, (span + WIN - 1) // WIN, window, 0)
            return carry

        lax.fori_loop(0, group, one_tile, 0)

    @pl.when(step >= steps)
    def _():
        lane = iota((slots, 128), 1)

        def one_expert(sub, carry):
            e = (step - steps) * group + sub
            for b in range(2):
                j = info_ref[b]
                kept = iota((slots, 1), 0) < start_ref[j, e, steps * group + 1]
                x = jnp.where(kept, xs_ref[b, e, 0:slots, :].astype(f32), 0.0)
                d = jnp.where(kept, ds_ref[b, e, 0:slots, :].astype(f32), 0.0)
                x = x.astype(bf16)
                x_ref[sub, b * slots:(b + 1) * slots, :] = x
                z = nn(x, wr3_ref[...])
                other = other_ref[j].T[0:slots, :]
                other = rsum(keep(iota((slots, n_local), 1) == e, other))
                name = lane % n_experts
                here = rsum(keep(name == info_ref[2] + e, z))
                there = rsum(keep(name == other.astype(jnp.int32), z))
                g = jax.nn.sigmoid(here - there)
                c_ref[sub, b * slots:(b + 1) * slots, :] = (g * (OUT_SCALE * d)).astype(bf16)
            return carry

        lax.fori_loop(0, group, one_expert, 0)


def act(ab, du):
    ff = du.shape[1]
    a, b = ab[:, :ff], ab[:, ff:]
    sig = jax.nn.sigmoid(a)
    silu = a * sig
    u = (silu * b).astype(bf16)
    da = (du * b * sig * (1.0 + a * (1.0 - sig))).astype(bf16)
    db = (du * silu).astype(bf16)
    return u, jnp.concatenate([da, db], axis=1)


def grad_kernel(accumulate, xa_ref, xb_ref, ca_ref, cb_ref, w13_ref, w2_ref, *refs):
    g1_ref, g3_ref, g2_ref = refs[-3:]
    ff = w2_ref.shape[1]
    d13, d2 = None, None
    for x_ref, c_ref in ((xa_ref, ca_ref), (xb_ref, cb_ref)):
        x, c = x_ref[0], c_ref[0]
        u, dab = act(nn(x, w13_ref[0]), nt(c, w2_ref[0]))
        p13, p2 = tn(x, dab), tn(u, c)
        d13, d2 = (p13, p2) if d13 is None else (d13 + p13, d2 + p2)
    if accumulate:
        g1_ref[0] = refs[0][0] + d13[:, :ff]
        g3_ref[0] = refs[1][0] + d13[:, ff:]
        g2_ref[0] = refs[2][0] + d2
    else:
        g1_ref[0] = d13[:, :ff]
        g3_ref[0] = d13[:, ff:]
        g2_ref[0] = d2


def row_kernel(slots, xa_ref, xb_ref, ca_ref, cb_ref, wo_ref, w2o_ref, wp_ref, w2p_ref, *r_refs):
    for q, (x_ref, c_ref) in enumerate(((xa_ref, ca_ref), (xb_ref, cb_ref))):
        x, c = x_ref[0], c_ref[0]
        y, dx = None, None
        for w_ref, v_ref in ((wo_ref, w2o_ref), (wp_ref, w2p_ref)):
            u, dab = act(nn(x, w_ref[0]), nt(c, v_ref[0]))
            py, pdx = nn(u, v_ref[0]), nt(dab, w_ref[0])
            y, dx = (py, pdx) if y is None else (y + py, dx + pdx)
        y, dx = y.astype(bf16), dx.astype(bf16)
        for b in range(2):
            if len(r_refs) == 8:
                r_refs[2 * q + b][0] = y[b * slots:(b + 1) * slots]
                r_refs[4 + 2 * q + b][0] = dx[b * slots:(b + 1) * slots]
            else:
                r_refs[2 * q + b][0, 0] = y[b * slots:(b + 1) * slots]
                r_refs[2 * q + b][0, 1] = dx[b * slots:(b + 1) * slots]


def names_of(groups, r_refs, part):
    names = []
    for gi, (lo, hi) in enumerate(groups):
        for q in range(4):
            ref = r_refs[4 * gi + q]
            for el in range(hi - lo):
                if len(ref.shape) == 4:
                    names.append((q, lo + el, lambda at, ref=ref, el=el: ref[el, part, pl.ds(at, 16), :]))
                else:
                    names.append((q, lo + el, lambda at, ref=ref, el=el: ref[el, pl.ds(at, 16), :]))
    return names


def fetch(names, w, slots, n_local, info_ref, win_ref, dst_ref):
    step = pl.program_id(0) + info_ref[4]
    for i, (q, el, read) in enumerate(names):
        first = win_ref[step, info_ref[q] * n_local + el]
        for piece in range(0, WIN, 16):
            at = pl.multiple_of(jnp.minimum(first + w * WIN + piece, slots - 16), 16)
            dst_ref[i * WIN + piece:i * WIN + piece + 16, :] = read(at)


def column(groups, n_local):
    width = 4 * sum(hi - lo for lo, hi in groups) * WIN
    lane = iota((1, width), 1)
    out, done = jnp.zeros((1, width), jnp.int32), 0
    for lo, hi in groups:
        for q in range(4):
            size = (hi - lo) * WIN
            out = jnp.where((lane >= done) & (lane < done + size), lane - done + (q * n_local + lo) * WIN, out)
            done += size
    return out.astype(f32)


def masks(code, w, col):
    if isinstance(w, int):
        return [ind(col == v) for v in cols(code, 2, 3)]
    low = (w * WIN).astype(f32)
    out = []
    for k in range(2):
        base, rel = cols(code, 7 + k, 9 + k)
        at = jnp.where((rel >= low) & (rel < low + WIN), base + rel - low, -1.0)
        out.append(ind(col == at))
    return out


def collect_y(code, w, col, rows_ref):
    return nn(jnp.concatenate(masks(code, w, col), axis=0).astype(bf16), rows_ref[...])


def collect_dx(code, w, col, rows_ref):
    m0, m1 = masks(code, w, col)
    return nn((m0 + m1).astype(bf16), rows_ref[...])


def further(info_ref, win_ref, body):
    n_win = win_ref[pl.program_id(0) + info_ref[4], win_ref.shape[1] - 1]

    @pl.when(n_win > 1)
    def _():
        def run(w, carry):
            body(w)
            return carry

        lax.fori_loop(1, n_win, run, 0)


def combine_kernel(groups, slots, n_local, info_ref, win_ref, code_ref, *refs):
    n_r = 4 * len(groups)
    y0_ref, y1_ref, dx_ref, rows_ref = refs[n_r:]
    code = code_ref[...]
    rows = code.shape[0]
    col = column(groups, n_local)

    def collect(w):
        fetch(names_of(groups, refs[:n_r], 0), w, slots, n_local, info_ref, win_ref, rows_ref.at[0])
        fetch(names_of(groups, refs[:n_r], 1), w, slots, n_local, info_ref, win_ref, rows_ref.at[1])
        return collect_y(code, w, col, rows_ref.at[0]), collect_dx(code, w, col, rows_ref.at[1])

    y, dx = collect(0)
    y0_ref[...] = y[:rows].astype(bf16)
    y1_ref[...] = y[rows:].astype(bf16)
    dx_ref[...] = dx

    def more(w):
        y, dx = collect(w)
        y0_ref[...] = (y0_ref[...].astype(f32) + y[:rows]).astype(bf16)
        y1_ref[...] = (y1_ref[...].astype(f32) + y[rows:]).astype(bf16)
        dx_ref[...] = dx_ref[...] + dx

    further(info_ref, win_ref, more)


def final_y_kernel(groups, slots, n_local, info_ref, win_ref, code_ref, *refs):
    n_r = 4 * len(groups)
    y0_ref, y1_ref, h_ref, d_ref, p_ref, coef_ref, stat_ref, out_ref, dz_ref, dr_ref, rows_ref, y_ref = refs[n_r:]
    code, p = code_ref[...], p_ref[...]
    n_experts = p.shape[1]
    rows = code.shape[0]
    col = column(groups, n_local)

    def collect(w):
        fetch(names_of(groups, refs[:n_r], 0), w, slots, n_local, info_ref, win_ref, rows_ref)
        return collect_y(code, w, col, rows_ref)

    y_ref[...] = jnp.zeros_like(y_ref)

    def more(w):
        y_ref[...] = y_ref[...] + collect(w)

    further(info_ref, win_ref, more)
    y = y_ref[...] + collect(0)
    y0 = y0_ref[...].astype(f32) + y[:rows]
    y1 = y1_ref[...].astype(f32) + y[rows:]
    e0, e1, g0, g1, s = cols(code, 0, 1, 4, 5, 6)
    h = h_ref[...]
    m = OUT_SCALE * d_ref[...].astype(f32)
    out_ref[...] = (h.astype(f32) + OUT_SCALE * (g0 * y0 + g1 * y1)).astype(bf16)
    dg0 = rsum(m * y0)
    dg1 = rsum(m * y1)
    mean = g0 * dg0 + g1 * dg1
    lane = iota(p.shape, 1).astype(f32)
    dp = (keep(lane == e0, (dg0 - mean) / s) + keep(lane == e1, (dg1 - mean) / s)
          + coef_ref[...])
    dz = p * (dp - rsum(p * dp))
    dz_ref[...] = dz
    z3 = split3(dz)
    part = tn(z3[0], h) + (tn(z3[1], h) + tn(z3[2], h))

    @pl.when(pl.program_id(0) == 0)
    def _():
        dr_ref[...] = jnp.zeros_like(dr_ref)
        dr_ref[n_experts:n_experts + 1, 0:128] = stat_ref[1:2, :]

    dr_ref[0:n_experts, :] = dr_ref[0:n_experts, :] + part


def final_x_kernel(groups, slots, n_local, info_ref, win_ref, code_ref, *refs):
    n_r = 4 * len(groups)
    dx_ref, d_ref, dz_ref, wr_ref = refs[n_r:n_r + 4]
    dh_ref, rows_ref, x_ref, wt_ref = refs[-4:]
    code = code_ref[...]
    col = column(groups, n_local)

    @pl.when(pl.program_id(0) == 0)
    def _():
        wt_ref[...] = wr_ref[...].T

    def collect(w):
        fetch(names_of(groups, refs[:n_r], 1), w, slots, n_local, info_ref, win_ref, rows_ref)
        return collect_dx(code, w, col, rows_ref)

    x_ref[...] = dx_ref[...]

    def more(w):
        x_ref[...] = x_ref[...] + collect(w)

    further(info_ref, win_ref, more)
    dx = x_ref[...] + collect(0)
    z_hi, z_lo, _ = split3(dz_ref[...])
    w_hi, w_lo, _ = split3(wt_ref[...])
    back = nn(z_hi, w_hi) + (nn(z_lo, w_hi) + nn(z_hi, w_lo))
    dh_ref[...] = (d_ref[...].astype(f32) + dx + back).astype(bf16)


def solution(mesh):
    ep_size = mesh.shape["ep"]
    etp_size = mesh.shape["etp"]
    n_dev = ep_size * etp_size
    all_axes = ("ep", "etp")
    tok_spec = P(all_axes, None)
    gate_spec = P("ep", None, "etp")
    down_spec = P("ep", "etp", None)

    def permute(v, dep, detp):
        pairs = [(t * ep_size + o, (t ^ detp) * ep_size + (o ^ dep)) for t in range(etp_size) for o in range(ep_size)]
        return lax.ppermute(v, ("etp", "ep"), pairs)

    def kernel(body, **kw):
        return pl.pallas_call(body, compiler_params=params(), cost_estimate=cost(8e9), **kw)

    def layer(hidden, w_router, expert_ids, d_out, w_gate, w_up, w_down):
        tok_rows, d_model = hidden.shape
        n_experts = w_router.shape[1]
        n_local, _, ff = w_gate.shape
        n_tokens = tok_rows * n_dev
        capacity = (5 * n_tokens + 2 * n_experts - 1) // (2 * n_experts)
        slots = 7 * tok_rows // (2 * n_experts)
        ep, etp = lax.axis_index("ep"), lax.axis_index("etp")
        steps = tok_rows // TILE
        ep_info = jnp.stack([ep ^ q for q in range(4)] + [jnp.zeros_like(ep)]).astype(jnp.int32)
        sds = jax.ShapeDtypeStruct
        smem = pl.BlockSpec(memory_space=pltpu.SMEM)

        def whole(shape):
            return pl.BlockSpec(shape, lambda i: (0,) * len(shape))

        def tokens(width, start=0):
            return pl.BlockSpec((TILE, width), lambda i: (i + start, 0))

        def expert_block(shape, lo=0):
            return pl.BlockSpec((1,) + shape, lambda i: (i + lo,) + (0,) * len(shape))

        tile_ids = expert_ids.reshape(steps, TILE, 2).transpose(0, 2, 1).reshape(2 * steps, TILE)
        near_ids = [tile_ids] + [permute(tile_ids, r // etp_size, r % etp_size) for r in range(1, n_dev)]
        near_ids = jnp.stack(near_ids)
        rank = ep * etp_size + etp
        rank_info = jnp.concatenate([jnp.arange(n_dev, dtype=jnp.int32) ^ rank, (ep * n_local)[None]]).astype(jnp.int32)
        w13 = jnp.concatenate([w_gate, w_up], axis=2)

        hx, hy = permute(hidden, 2, 0), permute(hidden, 0, 1)
        dx_, dy_ = permute(d_out, 2, 0), permute(d_out, 0, 1)
        hd, dd = permute(hy, 2, 0), permute(dy_, 2, 0)
        core = lambda v: permute(v, 1, 0)
        pairs = ((0, 0), (1, 0), (0, 1), (1, 1))
        h_pairs = {pair: (v, core(v)) for pair, v in zip(pairs, (hidden, hx, hy, hd))}
        d_pairs = {pair: (v, core(v)) for pair, v in zip(pairs, (d_out, dx_, dy_, dd))}
        partner = [(permute(w13[lo:hi], 0, 1), permute(w_down[lo:hi], 0, 1)) for lo, hi in CHUNKS]

        per_block = lambda *shape: pl.BlockSpec((1,) + shape, lambda i: (i,) + (0,) * len(shape))
        slot_rows, others, starts, wr3 = kernel(
            functools.partial(slot_kernel, capacity, slots, n_local),
            grid=(n_dev,),
            in_specs=[smem, whole(near_ids.shape), whole((d_model, n_experts))],
            out_specs=[per_block(steps * n_local, TILE), per_block(n_local, TILE), per_block(n_local, 128), whole((d_model, 128))],
            out_shape=[sds((n_dev, steps * n_local, TILE), f32), sds((n_dev, n_local, TILE), f32),
                       sds((n_dev, n_local, 128), jnp.int32), sds((d_model, 128), bf16)],
            scratch_shapes=[pltpu.VMEM((n_local, 128), f32)],
        )(rank_info, near_ids, w_router)

        probs, code, wins, stats = kernel(
            functools.partial(route_kernel, n_experts, n_local),
            grid=(steps,),
            in_specs=[smem, tokens(d_model), whole((d_model, n_experts)), tokens(2)],
            out_specs=[tokens(n_experts), tokens(128), whole((8, 128)), whole((8, 128))],
            out_shape=[sds((tok_rows, n_experts), f32), sds((tok_rows, 128), f32), sds((8, 128), jnp.int32), sds((8, 128), f32)],
        )(ep_info, hidden, w_router, expert_ids)

        def gather(pair):
            x, t = pair
            info = jnp.stack([(ep ^ (2 * x)) * etp_size + (etp ^ t), (ep ^ (2 * x + 1)) * etp_size + (etp ^ t), ep * n_local]).astype(jnp.int32)
            block = sds((n_local, 2 * slots, d_model), bf16)
            fills = steps // GROUP
            tile = pl.BlockSpec((GROUP * TILE, d_model), lambda i: (jnp.minimum(i, fills - 1), 0))
            out = pl.BlockSpec((GROUP, 2 * slots, d_model), lambda i: (jnp.maximum(i - fills, 0), 0, 0))
            return kernel(
                functools.partial(gather_kernel, slots, n_local, n_experts),
                grid=(fills + n_local // GROUP,),
                in_specs=[smem, smem, whole(slot_rows.shape), whole(others.shape), whole(wr3.shape)] + [tile] * 4,
                out_specs=[out] * 2,
                out_shape=[block, block],
                scratch_shapes=[pltpu.VMEM((n_local * WIN, TILE), bf16)] + [pltpu.VMEM((2, n_local, slots + 64, d_model), bf16)] * 2,
            )(info, starts, slot_rows, others, wr3, *h_pairs[pair], *d_pairs[pair])

        rows = {pair: gather(pair) for pair in h_pairs}

        def grads(first, second, acc, lo, hi):
            (xa, ca), (xb, cb) = rows[first], rows[second]
            at = lambda shape: expert_block(shape, lo)
            g13, g2 = at((d_model, ff)), at((ff, d_model))
            return kernel(
                functools.partial(grad_kernel, bool(acc)),
                grid=(hi - lo,),
                in_specs=[at((2 * slots, d_model))] * 4 + [at((d_model, 2 * ff)), at((ff, d_model))] + [g13, g13, g2][:len(acc)],
                out_specs=[g13, g13, g2],
                out_shape=[sds((n_local, d_model, ff), f32)] * 2 + [sds((n_local, ff, d_model), f32)],
                input_output_aliases={6 + k: k for k in range(len(acc))},
            )(xa, xb, ca, cb, w13, w_down, *acc)

        grad = grads((0, 0), (1, 0), (), 0, n_local)
        grad = grads((0, 1), (1, 1), tuple(grad), 0, n_local // 2)
        g_gate, g_up, g_down = grads((0, 1), (1, 1), tuple(grad), n_local // 2, n_local)

        def back(index):
            lo, hi = CHUNKS[index]
            (xa, ca), (xb, cb) = rows[(0, 0)], rows[(1, 0)]
            at = lambda shape: expert_block(shape, lo)
            outs = kernel(
                functools.partial(row_kernel, slots),
                grid=(hi - lo,),
                in_specs=[at((2 * slots, d_model))] * 4 + [at((d_model, 2 * ff)), at((ff, d_model)),
                          expert_block((d_model, 2 * ff)), expert_block((ff, d_model))],
                out_specs=[expert_block((slots, d_model))] * 8 if index >= split else [expert_block((2, slots, d_model))] * 4,
                out_shape=[sds((hi - lo, slots, d_model), bf16)] * 8 if index >= split else [sds((hi - lo, 2, slots, d_model), bf16)] * 4,
            )(xa, xb, ca, cb, w13, w_down, *partner[index])
            return [outs[i] if i % 4 == 0 else permute(outs[i], i % 4, 0) for i in range(len(outs))]

        last = len(CHUNKS) - 1
        split = last - 1
        returned = [back(i) for i in range(len(CHUNKS))]
        total = jnp.sum((near_ids.reshape(-1)[:, None] == jnp.arange(n_experts)[None, :]).astype(f32), axis=0)[None, :]
        coef = (AUX_COEF * n_experts / n_tokens / (2 * n_tokens)) * total

        def token_kernel(body, chunk_ids, arrays, extra, extra_specs, out_specs, out_shape, scratch,
                         start=0, count=steps, **kw):
            groups = tuple(CHUNKS[i] for i in chunk_ids)
            return kernel(
                functools.partial(body, groups, slots, n_local),
                grid=(count,),
                in_specs=[smem, smem, tokens(128, start=start)] + [whole(r.shape) for r in arrays] + extra_specs,
                out_specs=out_specs, out_shape=out_shape, scratch_shapes=scratch,
                **kw,
            )(ep_info.at[4].add(start), wins, code, *arrays, *extra)

        wide = tokens(d_model)
        width = lambda ids: 4 * sum(CHUNKS[i][1] - CHUNKS[i][0] for i in ids) * WIN
        early = range(split - 1)
        late = (split - 1, split, last)
        y0, y1, dxs = token_kernel(
            combine_kernel, early, [r for i in early for r in returned[i]], (), [],
            [wide] * 3, [sds((tok_rows, d_model), bf16)] * 2 + [sds((tok_rows, d_model), f32)],
            [pltpu.VMEM((2, width(early), d_model), bf16)])
        half = lambda k: [r for i in late for r in (returned[i] if len(returned[i]) == 4 else returned[i][4 * k:4 * k + 4])]
        output, dz, d_rt = token_kernel(
            final_y_kernel, late, half(0), (y0, y1, hidden, d_out, probs, coef, stats),
            [wide] * 4 + [tokens(n_experts), whole((1, n_experts)), whole((8, 128))],
            [wide, tokens(n_experts), whole((n_experts + 8, d_model))],
            [sds((tok_rows, d_model), bf16), sds((tok_rows, n_experts), f32), sds((n_experts + 8, d_model), f32)],
            [pltpu.VMEM((width(late), d_model), bf16), pltpu.VMEM((2 * TILE, d_model), f32)])
        mid = steps // 2
        d_hidden = []
        for start in (0, mid):
            wide = tokens(d_model, start)
            kw = {"input_output_aliases": {3 + len(half(1)) + 4: 0}} if d_hidden else {}
            d_hidden = token_kernel(
                final_x_kernel, late, half(1), (dxs, d_out, dz, w_router, *d_hidden),
                [wide] * 2 + [tokens(n_experts, start), whole((d_model, n_experts))] + [wide] * len(d_hidden),
                [wide], [sds((tok_rows, d_model), bf16)],
                [pltpu.VMEM((width(late), d_model), bf16), pltpu.VMEM((TILE, d_model), f32), pltpu.VMEM((n_experts, d_model), f32)],
                start, mid, **kw)
        (d_hidden,) = d_hidden
        for dep, detp in ((1, 0), (2, 0), (0, 1)):
            d_rt = d_rt + permute(d_rt, dep, detp)
        d_router = d_rt[:n_experts].T
        route_frac = total[0] / (2 * n_tokens)
        aux_loss = AUX_COEF * n_experts * jnp.sum(route_frac * (d_rt[n_experts, :n_experts] / n_tokens))
        return output, d_hidden, d_router, aux_loss, g_gate, g_up, g_down


    return jax.shard_map(layer, mesh=mesh, in_specs=(tok_spec, P(), tok_spec, tok_spec, gate_spec, gate_spec, down_spec), out_specs=(tok_spec, tok_spec, P(), P(), gate_spec, gate_spec, down_spec), check_vma=False)
```

```python
import functools
import jax
import jax.numpy as jnp
from jax import lax
from jax.experimental import pallas as pl
from jax.experimental.pallas import tpu as pltpu
from jax.sharding import PartitionSpec as P

AUX_COEF = 0.01
OUT_SCALE = 2.0
SIZES = (2, 2, 1, 1, 1, 1)
CHUNKS = tuple((sum(SIZES[:i]), sum(SIZES[:i]) + n) for i, n in enumerate(SIZES))

f32, bf16 = jnp.float32, jnp.bfloat16
TILE = 256
GROUP = 2
WIN = 48


def nn(a, b):
    return jnp.dot(a, b, preferred_element_type=f32)


def nt(a, b):
    return lax.dot_general(a, b, (((1,), (1,)), ((), ())), preferred_element_type=f32)


def tn(a, b):
    return lax.dot_general(a, b, (((0,), (0,)), ((), ())), preferred_element_type=f32)


def split3(v):
    hi = v.astype(bf16)
    rest = v - hi.astype(f32)
    mid = rest.astype(bf16)
    return hi, mid, (rest - mid.astype(f32)).astype(bf16)


def ind(mask):
    return jnp.where(mask, 1.0, 0.0).astype(f32)


def keep(mask, v):
    return jnp.where(mask, v, 0.0)


def rsum(v):
    return jnp.sum(v, axis=1, keepdims=True)


def csum(v):
    return jnp.sum(v, axis=0, keepdims=True)


def cols(v, *at):
    return [v[:, k:k + 1] for k in at]


def iota(shape, dim):
    return lax.broadcasted_iota(jnp.int32, shape, dim)


def params(**kw):
    return pltpu.CompilerParams(vmem_limit_bytes=63 * 2**20, **kw)


def cost(flops):
    return pl.CostEstimate(flops=int(flops), bytes_accessed=1 << 20, transcendentals=0)


def route_kernel(n_experts, n_local, info_ref, h_ref, wr_ref, ids_ref, p_ref, code_ref, win_ref, stat_ref):
    step = pl.program_id(0)

    @pl.when(step == 0)
    def _():
        stat_ref[...] = jnp.zeros_like(stat_ref)
        win_ref[...] = jnp.zeros_like(win_ref)

    w_hi, w_mid, w_lo = split3(wr_ref[...])
    h = h_ref[...]
    z = (nn(h, w_lo) + nn(h, w_mid)) + nn(h, w_hi)
    z = jnp.exp(z - jnp.max(z, axis=1, keepdims=True))
    p = z / rsum(z)
    p_ref[...] = p
    ids = ids_ref[...]
    lane = iota((TILE, n_experts), 1)
    e0, e1 = cols(ids, 0, 1)
    m0, m1 = lane == e0, lane == e1
    hist = ind(m0 | m1)
    before = (iota((TILE, TILE), 1) < iota((TILE, TILE), 0)).astype(f32).astype(bf16)
    seen = stat_ref[0:1, 0:n_experts]
    after = seen + csum(hist)
    start = jnp.floor(seen * (1.0 / 16)) * 16
    n_win = jnp.max(jnp.floor((after - start + (WIN - 1)) * (1.0 / WIN) + 1e-3), axis=1, keepdims=True)
    rank = nn(before, hist.astype(bf16)) + seen
    pick = lambda m, v: rsum(keep(m, v))
    p0, p1 = pick(m0, p), pick(m1, p)
    s = p0 + p1
    wide = iota((TILE, 128), 1)
    code = jnp.zeros((TILE, 128), f32)
    rel = rank - start
    name = iota((1, n_experts), 1)
    base = ((((name // n_local) ^ info_ref[0]) * n_local + name % n_local) * WIN).astype(f32)
    at = jnp.where(rel < WIN, base + rel, -1.0)
    spread = jnp.zeros_like(rel) + base
    for k, v in enumerate((e0.astype(f32), e1.astype(f32), pick(m0, at), pick(m1, at), p0 / s, p1 / s, s,
                           pick(m0, spread), pick(m1, spread), pick(m0, rel), pick(m1, rel))):
        code = jnp.where(wide == k, v, code)
    code_ref[...] = code
    win_ref[pl.ds(step, 1), 0:n_experts] = start.astype(jnp.int32)
    win_ref[pl.ds(step, 1), 127:128] = n_win.astype(jnp.int32)
    stat_ref[0:1, 0:n_experts] = after
    stat_ref[1:2, 0:n_experts] = stat_ref[1:2, 0:n_experts] + csum(p)


def slot_kernel(capacity, slots, n_local, info_ref, wr_ref, *refs):
    slot_ref, other_ref, start_ref, wr3_ref, total_ref, ids_ref = refs[-6:]

    @pl.when(pl.program_id(0) == 0)
    def _():
        total_ref[...] = jnp.zeros_like(total_ref)
        wr3_ref[...] = jnp.zeros_like(wr3_ref)
        for k, ref in enumerate(refs[:-6]):
            ids_ref[k] = ref[...]
        width = wr_ref.shape[1]
        for k, piece in enumerate(split3(wr_ref[...])):
            wr3_ref[:, k * width:(k + 1) * width] = piece

    steps = ids_ref.shape[1] // 2
    near = info_ref[pl.program_id(0)]
    expert = iota((n_local, TILE), 0) + info_ref[info_ref.shape[0] - 1]
    before = (iota((TILE, TILE), 0) < iota((TILE, TILE), 1)).astype(f32).astype(bf16)
    row = iota((TILE, TILE), 0).astype(f32)
    lane = iota((n_local, 128), 1)
    carry = jnp.zeros((n_local, 1), f32)
    starts = jnp.zeros((n_local, 128), f32)
    other = jnp.zeros((n_local, TILE), f32)
    for i in range(steps):
        e0, e1 = ids_ref[near, 2 * i:2 * i + 1, :], ids_ref[near, 2 * i + 1:2 * i + 2, :]
        m0, m1 = expert == e0, expert == e1
        hit = ind(m0 | m1)
        rank = nn(hit.astype(bf16), before) + carry
        slot_ref[0, i * n_local:(i + 1) * n_local, :] = jnp.where(m0 | m1, rank, -1.0)
        starts = jnp.where(lane == i, carry, starts)
        for m, e in ((m0, e1), (m1, e0)):
            pos = csum(keep(m, rank + 1.0)) - 1.0
            one = ind(row == pos).astype(bf16)
            other = other + nt(keep(m, e.astype(f32)).astype(bf16), one)
        carry = carry + rsum(hit)
    other_ref[0] = other
    prefix = total_ref[:, 0:1]
    room = jnp.clip(capacity - prefix, 0.0, float(slots))
    starts = jnp.where(lane == steps, carry, jnp.where(lane == steps + 1, jnp.minimum(room, carry), starts))
    start_ref[0] = starts.astype(jnp.int32)
    total_ref[...] = total_ref[...] + carry


def gather_kernel(slots, n_local, n_experts, info_ref, start_ref, slot_ref, other_ref, wr3_ref, ha_ref, hb_ref, da_ref, db_ref,
                  x_ref, c_ref, m_ref, xs_ref, ds_ref):
    step = pl.program_id(0)
    group = x_ref.shape[0]
    steps = pl.num_programs(0) - n_local // group

    @pl.when(step < steps)
    def _():
        row = iota((WIN, TILE), 0)

        def one_tile(sub, carry):
            tile = step * group + sub
            part = pl.ds(pl.multiple_of(sub * TILE, TILE), TILE)
            for b, (h_ref, d_ref) in enumerate(((ha_ref, da_ref), (hb_ref, db_ref))):
                j = info_ref[b]
                first = [(start_ref[j, e, tile] // 16) * 16 for e in range(n_local)]
                span = functools.reduce(jnp.maximum, [start_ref[j, e, tile + 1] - first[e] for e in range(n_local)])

                def window(w, carry):
                    for e in range(n_local):
                        slot = slot_ref[j, pl.ds(tile * n_local + e, 1), :]
                        hit = (row + (first[e] + w * WIN)).astype(f32) == slot
                        m_ref[e * WIN:(e + 1) * WIN, :] = ind(hit).astype(bf16)
                    m = m_ref[...]
                    for src, dst in ((h_ref, xs_ref), (d_ref, ds_ref)):
                        r = nn(m, src[part, :]).astype(bf16)
                        for e in range(n_local):
                            at = pl.multiple_of(jnp.minimum(first[e] + w * WIN, slots + 16), 16)
                            old = dst[b, e, pl.ds(at, 16), :]
                            older = iota((16, 1), 0) + at < start_ref[j, e, tile]
                            head = r[e * WIN:e * WIN + 16].astype(f32)
                            dst[b, e, pl.ds(at, 16), :] = jnp.where(older, old.astype(f32), head).astype(bf16)
                            dst[b, e, pl.ds(pl.multiple_of(at + 16, 16), WIN - 16), :] = r[e * WIN + 16:(e + 1) * WIN]
                    return carry

                lax.fori_loop(0, (span + WIN - 1) // WIN, window, 0)
            return carry

        lax.fori_loop(0, group, one_tile, 0)

    @pl.when(step >= steps)
    def _():
        lane = iota((slots, 128), 1)

        def one_expert(sub, carry):
            e = (step - steps) * group + sub
            for b in range(2):
                j = info_ref[b]
                kept = iota((slots, 1), 0) < start_ref[j, e, steps * group + 1]
                x = jnp.where(kept, xs_ref[b, e, 0:slots, :].astype(f32), 0.0)
                d = jnp.where(kept, ds_ref[b, e, 0:slots, :].astype(f32), 0.0)
                x = x.astype(bf16)
                x_ref[sub, b * slots:(b + 1) * slots, :] = x
                z = nn(x, wr3_ref[...])
                other = other_ref[j].T[0:slots, :]
                other = rsum(keep(iota((slots, n_local), 1) == e, other))
                name = lane % n_experts
                here = rsum(keep(name == info_ref[2] + e, z))
                there = rsum(keep(name == other.astype(jnp.int32), z))
                g = jax.nn.sigmoid(here - there)
                c_ref[sub, b * slots:(b + 1) * slots, :] = (g * (OUT_SCALE * d)).astype(bf16)
            return carry

        lax.fori_loop(0, group, one_expert, 0)


def act(ab, du):
    ff = du.shape[1]
    a, b = ab[:, :ff], ab[:, ff:]
    sig = jax.nn.sigmoid(a)
    silu = a * sig
    u = (silu * b).astype(bf16)
    da = (du * b * sig * (1.0 + a * (1.0 - sig))).astype(bf16)
    db = (du * silu).astype(bf16)
    return u, jnp.concatenate([da, db], axis=1)


def grad_kernel(accumulate, xa_ref, xb_ref, ca_ref, cb_ref, w13_ref, w2_ref, *refs):
    g1_ref, g3_ref, g2_ref = refs[-3:]
    ff = w2_ref.shape[1]
    d13, d2 = None, None
    for x_ref, c_ref in ((xa_ref, ca_ref), (xb_ref, cb_ref)):
        x, c = x_ref[0], c_ref[0]
        u, dab = act(nn(x, w13_ref[0]), nt(c, w2_ref[0]))
        p13, p2 = tn(x, dab), tn(u, c)
        d13, d2 = (p13, p2) if d13 is None else (d13 + p13, d2 + p2)
    if accumulate:
        g1_ref[0] = refs[0][0] + d13[:, :ff]
        g3_ref[0] = refs[1][0] + d13[:, ff:]
        g2_ref[0] = refs[2][0] + d2
    else:
        g1_ref[0] = d13[:, :ff]
        g3_ref[0] = d13[:, ff:]
        g2_ref[0] = d2


def row_kernel(slots, xa_ref, xb_ref, ca_ref, cb_ref, wo_ref, w2o_ref, wp_ref, w2p_ref, *r_refs):
    for q, (x_ref, c_ref) in enumerate(((xa_ref, ca_ref), (xb_ref, cb_ref))):
        x, c = x_ref[0], c_ref[0]
        y, dx = None, None
        for w_ref, v_ref in ((wo_ref, w2o_ref), (wp_ref, w2p_ref)):
            u, dab = act(nn(x, w_ref[0]), nt(c, v_ref[0]))
            py, pdx = nn(u, v_ref[0]), nt(dab, w_ref[0])
            y, dx = (py, pdx) if y is None else (y + py, dx + pdx)
        y, dx = y.astype(bf16), dx.astype(bf16)
        for b in range(2):
            if len(r_refs) == 8:
                r_refs[2 * q + b][0] = y[b * slots:(b + 1) * slots]
                r_refs[4 + 2 * q + b][0] = dx[b * slots:(b + 1) * slots]
            else:
                r_refs[2 * q + b][0, 0] = y[b * slots:(b + 1) * slots]
                r_refs[2 * q + b][0, 1] = dx[b * slots:(b + 1) * slots]


def names_of(groups, r_refs, part):
    names = []
    for gi, (lo, hi) in enumerate(groups):
        for q in range(4):
            ref = r_refs[4 * gi + q]
            for el in range(hi - lo):
                if len(ref.shape) == 4:
                    names.append((q, lo + el, lambda at, ref=ref, el=el: ref[el, part, pl.ds(at, 16), :]))
                else:
                    names.append((q, lo + el, lambda at, ref=ref, el=el: ref[el, pl.ds(at, 16), :]))
    return names


def fetch(names, w, slots, n_local, info_ref, win_ref, dst_ref):
    step = pl.program_id(0) + info_ref[4]
    for i, (q, el, read) in enumerate(names):
        first = win_ref[step, info_ref[q] * n_local + el]
        for piece in range(0, WIN, 16):
            at = pl.multiple_of(jnp.minimum(first + w * WIN + piece, slots - 16), 16)
            dst_ref[i * WIN + piece:i * WIN + piece + 16, :] = read(at)


def column(groups, n_local):
    width = 4 * sum(hi - lo for lo, hi in groups) * WIN
    lane = iota((1, width), 1)
    out, done = jnp.zeros((1, width), jnp.int32), 0
    for lo, hi in groups:
        for q in range(4):
            size = (hi - lo) * WIN
            out = jnp.where((lane >= done) & (lane < done + size), lane - done + (q * n_local + lo) * WIN, out)
            done += size
    return out.astype(f32)


def masks(code, w, col):
    if isinstance(w, int):
        return [ind(col == v) for v in cols(code, 2, 3)]
    low = (w * WIN).astype(f32)
    out = []
    for k in range(2):
        base, rel = cols(code, 7 + k, 9 + k)
        at = jnp.where((rel >= low) & (rel < low + WIN), base + rel - low, -1.0)
        out.append(ind(col == at))
    return out


def collect_y(code, w, col, rows_ref):
    return nn(jnp.concatenate(masks(code, w, col), axis=0).astype(bf16), rows_ref[...])


def collect_dx(code, w, col, rows_ref):
    m0, m1 = masks(code, w, col)
    return nn((m0 + m1).astype(bf16), rows_ref[...])


def further(info_ref, win_ref, body):
    n_win = win_ref[pl.program_id(0) + info_ref[4], win_ref.shape[1] - 1]

    @pl.when(n_win > 1)
    def _():
        def run(w, carry):
            body(w)
            return carry

        lax.fori_loop(1, n_win, run, 0)


def combine_kernel(groups, slots, n_local, info_ref, win_ref, code_ref, *refs):
    n_r = 4 * len(groups)
    y0_ref, y1_ref, dx_ref, rows_ref = refs[n_r:]
    code = code_ref[...]
    rows = code.shape[0]
    col = column(groups, n_local)

    def collect(w):
        fetch(names_of(groups, refs[:n_r], 0), w, slots, n_local, info_ref, win_ref, rows_ref.at[0])
        fetch(names_of(groups, refs[:n_r], 1), w, slots, n_local, info_ref, win_ref, rows_ref.at[1])
        return collect_y(code, w, col, rows_ref.at[0]), collect_dx(code, w, col, rows_ref.at[1])

    y, dx = collect(0)
    y0_ref[...] = y[:rows].astype(bf16)
    y1_ref[...] = y[rows:].astype(bf16)
    dx_ref[...] = dx

    def more(w):
        y, dx = collect(w)
        y0_ref[...] = (y0_ref[...].astype(f32) + y[:rows]).astype(bf16)
        y1_ref[...] = (y1_ref[...].astype(f32) + y[rows:]).astype(bf16)
        dx_ref[...] = dx_ref[...] + dx

    further(info_ref, win_ref, more)


def final_y_kernel(groups, slots, n_local, info_ref, win_ref, code_ref, *refs):
    n_r = 4 * len(groups)
    y0_ref, y1_ref, h_ref, d_ref, p_ref, coef_ref, stat_ref, out_ref, dz_ref, dr_ref, rows_ref, y_ref = refs[n_r:]
    code, p = code_ref[...], p_ref[...]
    n_experts = p.shape[1]
    rows = code.shape[0]
    col = column(groups, n_local)

    def collect(w):
        fetch(names_of(groups, refs[:n_r], 0), w, slots, n_local, info_ref, win_ref, rows_ref)
        return collect_y(code, w, col, rows_ref)

    y_ref[...] = jnp.zeros_like(y_ref)

    def more(w):
        y_ref[...] = y_ref[...] + collect(w)

    further(info_ref, win_ref, more)
    y = y_ref[...] + collect(0)
    y0 = y0_ref[...].astype(f32) + y[:rows]
    y1 = y1_ref[...].astype(f32) + y[rows:]
    e0, e1, g0, g1, s = cols(code, 0, 1, 4, 5, 6)
    h = h_ref[...]
    m = OUT_SCALE * d_ref[...].astype(f32)
    out_ref[...] = (h.astype(f32) + OUT_SCALE * (g0 * y0 + g1 * y1)).astype(bf16)
    dg0 = rsum(m * y0)
    dg1 = rsum(m * y1)
    mean = g0 * dg0 + g1 * dg1
    lane = iota(p.shape, 1).astype(f32)
    dp = (keep(lane == e0, (dg0 - mean) / s) + keep(lane == e1, (dg1 - mean) / s)
          + coef_ref[...])
    dz = p * (dp - rsum(p * dp))
    dz_ref[...] = dz
    z3 = split3(dz)
    part = tn(z3[0], h) + (tn(z3[1], h) + tn(z3[2], h))

    @pl.when(pl.program_id(0) == 0)
    def _():
        dr_ref[...] = jnp.zeros_like(dr_ref)
        dr_ref[n_experts:n_experts + 1, 0:128] = stat_ref[1:2, :]

    dr_ref[0:n_experts, :] = dr_ref[0:n_experts, :] + part


def final_x_kernel(groups, slots, n_local, info_ref, win_ref, code_ref, *refs):
    n_r = 4 * len(groups)
    dx_ref, d_ref, dz_ref, wr_ref = refs[n_r:n_r + 4]
    dh_ref, rows_ref, x_ref, wt_ref = refs[-4:]
    code = code_ref[...]
    col = column(groups, n_local)

    @pl.when(pl.program_id(0) == 0)
    def _():
        wt_ref[...] = wr_ref[...].T

    def collect(w):
        fetch(names_of(groups, refs[:n_r], 1), w, slots, n_local, info_ref, win_ref, rows_ref)
        return collect_dx(code, w, col, rows_ref)

    x_ref[...] = dx_ref[...]

    def more(w):
        x_ref[...] = x_ref[...] + collect(w)

    further(info_ref, win_ref, more)
    dx = x_ref[...] + collect(0)
    z_hi, z_lo, _ = split3(dz_ref[...])
    w_hi, w_lo, _ = split3(wt_ref[...])
    back = nn(z_hi, w_hi) + (nn(z_lo, w_hi) + nn(z_hi, w_lo))
    dh_ref[...] = (d_ref[...].astype(f32) + dx + back).astype(bf16)


def solution(mesh):
    ep_size = mesh.shape["ep"]
    etp_size = mesh.shape["etp"]
    n_dev = ep_size * etp_size
    all_axes = ("ep", "etp")
    tok_spec = P(all_axes, None)
    gate_spec = P("ep", None, "etp")
    down_spec = P("ep", "etp", None)

    def permute(v, dep, detp):
        pairs = [(t * ep_size + o, (t ^ detp) * ep_size + (o ^ dep)) for t in range(etp_size) for o in range(ep_size)]
        return lax.ppermute(v, ("etp", "ep"), pairs)

    def kernel(body, **kw):
        return pl.pallas_call(body, compiler_params=params(), cost_estimate=cost(8e9), **kw)

    def layer(hidden, w_router, expert_ids, d_out, w_gate, w_up, w_down):
        tok_rows, d_model = hidden.shape
        n_experts = w_router.shape[1]
        n_local, _, ff = w_gate.shape
        n_tokens = tok_rows * n_dev
        capacity = (5 * n_tokens + 2 * n_experts - 1) // (2 * n_experts)
        slots = 7 * tok_rows // (2 * n_experts)
        ep, etp = lax.axis_index("ep"), lax.axis_index("etp")
        steps = tok_rows // TILE
        ep_info = jnp.stack([ep ^ q for q in range(4)] + [jnp.zeros_like(ep)]).astype(jnp.int32)
        sds = jax.ShapeDtypeStruct
        smem = pl.BlockSpec(memory_space=pltpu.SMEM)

        def whole(shape):
            return pl.BlockSpec(shape, lambda i: (0,) * len(shape))

        def tokens(width, start=0):
            return pl.BlockSpec((TILE, width), lambda i: (i + start, 0))

        def expert_block(shape, lo=0):
            return pl.BlockSpec((1,) + shape, lambda i: (i + lo,) + (0,) * len(shape))

        tile_ids = expert_ids.reshape(steps, TILE, 2).transpose(0, 2, 1).reshape(2 * steps, TILE)
        near_ids = [tile_ids] + [permute(tile_ids, r // etp_size, r % etp_size) for r in range(1, n_dev)]
        rank = ep * etp_size + etp
        rank_info = jnp.concatenate([jnp.arange(n_dev, dtype=jnp.int32) ^ rank, (ep * n_local)[None]]).astype(jnp.int32)
        w13 = jnp.concatenate([w_gate, w_up], axis=2)

        cut = tok_rows // 2
        h_lo, h_hi = hidden[:cut], hidden[cut:]
        hx = jnp.concatenate([permute(h_lo, 2, 0), permute(h_hi, 2, 0)])
        hy = jnp.concatenate([permute(h_lo, 0, 1), permute(h_hi, 0, 1)])
        dx_, dy_ = permute(d_out, 2, 0), permute(d_out, 0, 1)
        hd, dd = permute(hy, 2, 0), permute(dy_, 2, 0)
        core = lambda v: permute(v, 1, 0)
        pairs = ((0, 0), (1, 0), (0, 1), (1, 1))
        h_pairs = {pair: (v, core(v)) for pair, v in zip(pairs, (hidden, hx, hy, hd))}
        d_pairs = {pair: (v, core(v)) for pair, v in zip(pairs, (d_out, dx_, dy_, dd))}
        partner = [(permute(w13[lo:hi], 0, 1), permute(w_down[lo:hi], 0, 1)) for lo, hi in CHUNKS]

        per_block = lambda *shape: pl.BlockSpec((1,) + shape, lambda i: (i,) + (0,) * len(shape))
        slot_rows, others, starts, wr3 = kernel(
            functools.partial(slot_kernel, capacity, slots, n_local),
            grid=(n_dev,),
            in_specs=[smem, whole((d_model, n_experts))] + [whole(tile_ids.shape)] * n_dev,
            out_specs=[per_block(steps * n_local, TILE), per_block(n_local, TILE), per_block(n_local, 128), whole((d_model, 128))],
            out_shape=[sds((n_dev, steps * n_local, TILE), f32), sds((n_dev, n_local, TILE), f32),
                       sds((n_dev, n_local, 128), jnp.int32), sds((d_model, 128), bf16)],
            scratch_shapes=[pltpu.VMEM((n_local, 128), f32), pltpu.VMEM((n_dev, *tile_ids.shape), jnp.int32)],
        )(rank_info, w_router, *near_ids)

        probs, code, wins, stats = kernel(
            functools.partial(route_kernel, n_experts, n_local),
            grid=(steps,),
            in_specs=[smem, tokens(d_model), whole((d_model, n_experts)), tokens(2)],
            out_specs=[tokens(n_experts), tokens(128), whole((8, 128)), whole((8, 128))],
            out_shape=[sds((tok_rows, n_experts), f32), sds((tok_rows, 128), f32), sds((8, 128), jnp.int32), sds((8, 128), f32)],
        )(ep_info, hidden, w_router, expert_ids)

        def gather(pair):
            x, t = pair
            info = jnp.stack([(ep ^ (2 * x)) * etp_size + (etp ^ t), (ep ^ (2 * x + 1)) * etp_size + (etp ^ t), ep * n_local]).astype(jnp.int32)
            block = sds((n_local, 2 * slots, d_model), bf16)
            fills = steps // GROUP
            tile = pl.BlockSpec((GROUP * TILE, d_model), lambda i: (jnp.minimum(i, fills - 1), 0))
            out = pl.BlockSpec((GROUP, 2 * slots, d_model), lambda i: (jnp.maximum(i - fills, 0), 0, 0))
            return kernel(
                functools.partial(gather_kernel, slots, n_local, n_experts),
                grid=(fills + n_local // GROUP,),
                in_specs=[smem, smem, whole(slot_rows.shape), whole(others.shape), whole(wr3.shape)] + [tile] * 4,
                out_specs=[out] * 2,
                out_shape=[block, block],
                scratch_shapes=[pltpu.VMEM((n_local * WIN, TILE), bf16)] + [pltpu.VMEM((2, n_local, slots + 64, d_model), bf16)] * 2,
            )(info, starts, slot_rows, others, wr3, *h_pairs[pair], *d_pairs[pair])

        rows = {pair: gather(pair) for pair in h_pairs}

        def grads(first, second, acc, lo, hi):
            (xa, ca), (xb, cb) = rows[first], rows[second]
            at = lambda shape: expert_block(shape, lo)
            g13, g2 = at((d_model, ff)), at((ff, d_model))
            return kernel(
                functools.partial(grad_kernel, bool(acc)),
                grid=(hi - lo,),
                in_specs=[at((2 * slots, d_model))] * 4 + [at((d_model, 2 * ff)), at((ff, d_model))] + [g13, g13, g2][:len(acc)],
                out_specs=[g13, g13, g2],
                out_shape=[sds((n_local, d_model, ff), f32)] * 2 + [sds((n_local, ff, d_model), f32)],
                input_output_aliases={6 + k: k for k in range(len(acc))},
            )(xa, xb, ca, cb, w13, w_down, *acc)

        grad = grads((0, 0), (1, 0), (), 0, n_local)
        grad = grads((0, 1), (1, 1), tuple(grad), 0, n_local // 2)
        g_gate, g_up, g_down = grads((0, 1), (1, 1), tuple(grad), n_local // 2, n_local)

        def back(index):
            lo, hi = CHUNKS[index]
            (xa, ca), (xb, cb) = rows[(0, 0)], rows[(1, 0)]
            at = lambda shape: expert_block(shape, lo)
            outs = kernel(
                functools.partial(row_kernel, slots),
                grid=(hi - lo,),
                in_specs=[at((2 * slots, d_model))] * 4 + [at((d_model, 2 * ff)), at((ff, d_model)),
                          expert_block((d_model, 2 * ff)), expert_block((ff, d_model))],
                out_specs=[expert_block((slots, d_model))] * 8 if index >= split else [expert_block((2, slots, d_model))] * 4,
                out_shape=[sds((hi - lo, slots, d_model), bf16)] * 8 if index >= split else [sds((hi - lo, 2, slots, d_model), bf16)] * 4,
            )(xa, xb, ca, cb, w13, w_down, *partner[index])
            return [outs[i] if i % 4 == 0 else permute(outs[i], i % 4, 0) for i in range(len(outs))]

        last = len(CHUNKS) - 1
        split = last - 1
        returned = [back(i) for i in range(len(CHUNKS))]
        total = jnp.sum((jnp.concatenate(near_ids).reshape(-1)[:, None] == jnp.arange(n_experts)[None, :]).astype(f32), axis=0)[None, :]
        coef = (AUX_COEF * n_experts / n_tokens / (2 * n_tokens)) * total

        def token_kernel(body, chunk_ids, arrays, extra, extra_specs, out_specs, out_shape, scratch,
                         start=0, count=steps, **kw):
            groups = tuple(CHUNKS[i] for i in chunk_ids)
            return kernel(
                functools.partial(body, groups, slots, n_local),
                grid=(count,),
                in_specs=[smem, smem, tokens(128, start=start)] + [whole(r.shape) for r in arrays] + extra_specs,
                out_specs=out_specs, out_shape=out_shape, scratch_shapes=scratch,
                **kw,
            )(ep_info.at[4].add(start), wins, code, *arrays, *extra)

        wide = tokens(d_model)
        width = lambda ids: 4 * sum(CHUNKS[i][1] - CHUNKS[i][0] for i in ids) * WIN
        early = range(split - 1)
        late = (split - 1, split, last)
        y0, y1, dxs = token_kernel(
            combine_kernel, early, [r for i in early for r in returned[i]], (), [],
            [wide] * 3, [sds((tok_rows, d_model), bf16)] * 2 + [sds((tok_rows, d_model), f32)],
            [pltpu.VMEM((2, width(early), d_model), bf16)])
        half = lambda k: [r for i in late for r in (returned[i] if len(returned[i]) == 4 else returned[i][4 * k:4 * k + 4])]
        output, dz, d_rt = token_kernel(
            final_y_kernel, late, half(0), (y0, y1, hidden, d_out, probs, coef, stats),
            [wide] * 4 + [tokens(n_experts), whole((1, n_experts)), whole((8, 128))],
            [wide, tokens(n_experts), whole((n_experts + 8, d_model))],
            [sds((tok_rows, d_model), bf16), sds((tok_rows, n_experts), f32), sds((n_experts + 8, d_model), f32)],
            [pltpu.VMEM((width(late), d_model), bf16), pltpu.VMEM((2 * TILE, d_model), f32)])
        third = -(-steps // 3)
        d_hidden = []
        for start in range(0, steps, third):
            wide = tokens(d_model, start)
            kw = {"input_output_aliases": {3 + len(half(1)) + 4: 0}} if d_hidden else {}
            d_hidden = token_kernel(
                final_x_kernel, late, half(1), (dxs, d_out, dz, w_router, *d_hidden),
                [wide] * 2 + [tokens(n_experts, start), whole((d_model, n_experts))] + [wide] * len(d_hidden),
                [wide], [sds((tok_rows, d_model), bf16)],
                [pltpu.VMEM((width(late), d_model), bf16), pltpu.VMEM((TILE, d_model), f32), pltpu.VMEM((n_experts, d_model), f32)],
                start, min(third, steps - start), **kw)
        (d_hidden,) = d_hidden
        for dep, detp in ((1, 0), (2, 0), (0, 1)):
            d_rt = d_rt + permute(d_rt, dep, detp)
        d_router = d_rt[:n_experts].T
        route_frac = total[0] / (2 * n_tokens)
        aux_loss = AUX_COEF * n_experts * jnp.sum(route_frac * (d_rt[n_experts, :n_experts] / n_tokens))
        return output, d_hidden, d_router, aux_loss, g_gate, g_up, g_down


    return jax.shard_map(layer, mesh=mesh, in_specs=(tok_spec, P(), tok_spec, tok_spec, gate_spec, gate_spec, down_spec), out_specs=(tok_spec, tok_spec, P(), P(), gate_spec, gate_spec, down_spec), check_vma=False)
```
